32 devices in a mesh: dp: 2 (over x), expert: 4 (over z), seq: 4 (over y, core).
Axes of the slice: x: 2, y: 2, z: 4, core: 2. Of those that a mesh axis runs over, the one named last changes fastest.
Arguments:
- tokens: bfloat16 [4096, 1024], P(('dp', 'expert', 'seq')), parts along dimension 0, may hold values from -6 to 6
- picks: int32 [32, 4, 16], P(('dp', 'expert', 'seq')), parts along dimension 0, may hold values from 0 to 127, as said below
- gates: float32 [32, 4, 16], P(('dp', 'expert', 'seq')), parts along dimension 0, may hold values from 0.1 to 2
- counts: int32 [32, 4], P(('dp', 'expert', 'seq')), parts along dimension 0, may hold values from 1 to 16, as said below
- norm_in: float32 [1024], replicated, may hold values from 0.1 to 1.9
- norm_out: float32 [1024], replicated, may hold values from 0.1 to 1.9
- w_in: bfloat16 [4, 1024, 1408], P('expert'), may hold values from -0.1875 to 0.1875
- w_out: bfloat16 [4, 1408, 1024], P('expert'), may hold values from -0.15625 to 0.15625
- w_key: bfloat16 [1024, 512], replicated, may hold values from -0.1875 to 0.1875
- w_value: bfloat16 [1024, 512], replicated, may hold values from -0.1875 to 0.1875
- queries: bfloat16 [1024, 512], P(('dp', 'expert', 'seq')), parts along dimension 0, may hold values from -300 to 300
- w_proj: bfloat16 [512, 1024], replicated, may hold values from -0.25 to 0.25
Outputs:
- encoded: bfloat16 [4096, 1024], P(('dp', 'expert', 'seq')), parts along dimension 0
- dec_out: bfloat16 [1024, 1024], P(('dp', 'expert', 'seq')), parts along dimension 0
The draws below stay inside these ranges and needn't reach their ends.
There are 2 independent parts, one for each index of `dp`. The reference program is written for one: setup_inputs(seed, part) draws one part's arguments, and reference() takes and returns one part's arrays. A program takes and returns all parts, laid end to end along the dimension named above; an argument that names none is the same for every part. Nothing has to cross between parts.
Inputs may be any that keep to these rules, and one draw needn't show every extreme that they name: `picks`: for each source device and expert, 16 different row numbers of that device's 128 tokens. Slots c < counts are live, the rest are padding; some source device and expert has all 16 slots live.
All inputs are finite; a program needn't handle non-finite values.
Results may differ from the reference program's by a relative error of at most 0.015.
The reference program's roundings to bfloat16 on the way count: a program that leaves them out, or rounds other values in their place, can miss the bound.
Values may be sent and summed in bfloat16 or wider, within the bound.
A program may use at most 64 MiB of HBM per device.

```python
import math
import jax
import jax.numpy as jnp
from jax import lax

D = 1024
FF = 1408
HEADS = 8
TOK_DEV = 128
DEC_DEV = 32
EXPERTS = 4
CAP = 16
SOURCES = 16
TOKENS = 2048
DEC_TOKENS = 512
HQ = 512
N_EXPERT = 4
N_SEQ = 4


def draw_picks(key, part):
    subkeys = jax.random.split(jax.random.fold_in(key, 11), SOURCES * EXPERTS)

    def choose(subkey):
        return jax.random.permutation(subkey, TOK_DEV)[:CAP]
    chosen = jax.vmap(choose)(subkeys)
    return chosen.reshape(SOURCES, EXPERTS, CAP).astype(jnp.int32)


def draw_counts(key, part):
    first, second = jax.random.split(jax.random.fold_in(key, 23))
    drawn = jax.random.randint(first, (SOURCES * EXPERTS,), 1, CAP + 1, dtype=jnp.int32)
    position = jax.random.randint(second, (), 0, SOURCES * EXPERTS, dtype=jnp.int32)
    drawn = drawn.at[position].set(CAP)
    return drawn.reshape(SOURCES, EXPERTS).astype(jnp.int32)


def draw_queries(key, part):
    first = jax.random.fold_in(jax.random.fold_in(key, 37), 0)
    base = jnp.clip(jax.random.normal(first, (DEC_TOKENS, HQ), jnp.float32), -6.0, 6.0)
    return base.astype(jnp.bfloat16)


def levels(own_key, dims, pieces, low, largest):
    level, own = 1.0, jax.random.fold_in(own_key, 6)
    for dim, blocks in pieces:
        heights = jnp.exp(jax.random.uniform(jax.random.fold_in(own, dim), (blocks,), jnp.float32, low / len(pieces), largest / len(pieces)))
        level = level * jnp.repeat(heights, dims[dim] // blocks).reshape([-1 if axis == dim else 1 for axis in range(len(dims))])
    return level


def scatter_about(own_key, dims, scale, bound, shards=(), kind=jnp.bfloat16):
    array = jax.random.normal(own_key, dims, jnp.float32) * scale
    if len(shards) > 0:
        array = levels(own_key, dims, shards, -0.22, 0.18) * array
    return jnp.clip(array, min=-bound, max=bound).astype(kind)


def setup_inputs(seed: int = 0, part: int = 0) -> dict:
    key_of = jax.random.split(jax.random.key(seed), 13)
    part_splits = jax.random.split(jax.random.fold_in(key_of[12], part), 13)
    return {
        "tokens": scatter_about(part_splits[0], (TOKENS, D), 1.0, 6.0, ((0, 16),)),
        "picks": draw_picks(jax.random.fold_in(jax.random.fold_in(key_of[12], part), 71), part),
        "gates": jnp.clip(jnp.exp(math.log(2.0) - 2.9957323 * jax.random.uniform(part_splits[2], (SOURCES, EXPERTS, CAP), jnp.float32) ** levels(part_splits[2], (SOURCES, EXPERTS, CAP), ((0, 16),), -0.2, 0.2)), 0.1, 2.0),
        "counts": draw_counts(jax.random.fold_in(jax.random.fold_in(key_of[12], part), 71), part),
        "norm_in": jnp.clip(1.0 + 0.18 * jax.random.normal(key_of[4], (D,), jnp.float32), 0.1, 1.9),
        "norm_out": jnp.clip(1.0 + 0.18 * jax.random.normal(key_of[5], (D,), jnp.float32), 0.1, 1.9),
        "w_in": scatter_about(key_of[6], (EXPERTS, D, FF), D ** -0.5, 0.1875, ((0, 4),)),
        "w_out": scatter_about(key_of[7], (EXPERTS, FF, D), FF ** -0.5, 0.15625, ((0, 4),)),
        "w_key": scatter_about(key_of[8], (D, HQ), D ** -0.5, 0.1875),
        "w_value": scatter_about(key_of[9], (D, HQ), D ** -0.5, 0.1875),
        "queries": draw_queries(jax.random.fold_in(jax.random.fold_in(key_of[12], part), 71), part),
        "w_proj": scatter_about(key_of[11], (HQ, D), HQ ** -0.5, 0.25),
    }


EPSILON = 1e-06

def rms_norm(values, gain):
    mean_square = lax.optimization_barrier(jnp.mean(values * values, axis=-1, keepdims=True))
    return values * lax.rsqrt(mean_square + EPSILON) * gain

def reference(tokens, picks, gates, counts, norm_in, norm_out, w_in, w_out, w_key, w_value, queries, w_proj):
    model_width = tokens.shape[1]
    plain = tokens.astype(jnp.float32)
    normed = rms_norm(plain, norm_in.astype(jnp.float32)).astype(jnp.bfloat16)
    offsets = jnp.arange(SOURCES, dtype=jnp.int32) * TOK_DEV
    row_index = (picks + offsets[:, None, None]).astype(jnp.int32)

    def expert_apply(expert):
        chosen = jnp.take(normed, row_index[:, expert, :].reshape(-1), axis=0)
        hidden = jax.nn.gelu(jnp.dot(chosen, w_in[expert], preferred_element_type=jnp.float32), approximate=True).astype(jnp.bfloat16)
        return jnp.dot(hidden, w_out[expert], preferred_element_type=jnp.float32).astype(jnp.bfloat16)
    outputs = lax.map(expert_apply, jnp.arange(EXPERTS, dtype=jnp.int32))
    ordered = outputs.reshape(EXPERTS, SOURCES, CAP, model_width).transpose(1, 0, 2, 3)
    live = (jnp.arange(CAP, dtype=jnp.int32)[None, None, :] < counts[:, :, None]).astype(jnp.float32)
    slot_weight = gates.astype(jnp.float32) * live
    terms = ordered.astype(jnp.float32) * slot_weight[..., None]
    expert_sum = jnp.zeros((TOKENS, model_width), jnp.float32).at[row_index.reshape(-1)].add(terms.reshape(-1, model_width))
    mixed = plain + expert_sum
    encoded = rms_norm(mixed, norm_out.astype(jnp.float32)).astype(jnp.bfloat16)
    key_proj = jnp.dot(encoded, w_key, preferred_element_type=jnp.float32).astype(jnp.bfloat16)
    value_proj = jnp.dot(encoded, w_value, preferred_element_type=jnp.float32).astype(jnp.bfloat16)
    head_size = queries.shape[1] // HEADS
    seq_length = N_SEQ * TOK_DEV
    key_heads = key_proj.reshape(N_EXPERT, seq_length, HEADS, head_size)
    value_heads = value_proj.reshape(N_EXPERT, seq_length, HEADS, head_size)
    query_heads = queries.reshape(N_EXPERT, N_SEQ * DEC_DEV, HEADS, head_size)

    def attend(inputs):
        query_block, key_block, value_block = inputs
        scores = jnp.einsum('qhd,khd->qhk', query_block.astype(jnp.float32), key_block.astype(jnp.float32)) * head_size ** (-0.5)
        row_max = lax.optimization_barrier(jnp.max(scores, axis=-1, keepdims=True))
        weights = jnp.exp(scores - row_max)
        row_total = lax.optimization_barrier(jnp.sum(weights, axis=-1))
        rounded = lax.optimization_barrier(weights.astype(jnp.bfloat16)).astype(jnp.float32)
        context = jnp.einsum('qhk,khd->qhd', rounded, value_block.astype(jnp.float32)) / row_total[..., None]
        return context.astype(jnp.bfloat16)
    contexts = lax.map(attend, (query_heads, key_heads, value_heads))
    context = contexts.reshape(DEC_TOKENS, HEADS * head_size)
    dec_out = jnp.dot(context, w_proj, preferred_element_type=jnp.float32).astype(jnp.bfloat16)
    return (encoded, dec_out)
```

```python
import functools

import jax
import jax.numpy as jnp
from jax import lax
from jax.experimental import pallas as pl
from jax.experimental.pallas import tpu as pltpu
from jax.sharding import PartitionSpec as P

HEADS = 8
EPSILON = 1e-06
VMEM_BYTES = 67043328
MESH = pl.DeviceIdType.MESH
F32 = jnp.float32
BF16 = jnp.bfloat16


def rms_norm(values, gain):
    mean_square = jnp.mean(values * values, axis=-1, keepdims=True)
    return values * lax.rsqrt(mean_square + EPSILON) * gain


def gelu(v):
    return 0.5 * v * (1.0 + jnp.tanh(0.7978845608028654 * (v + 0.044715 * v * v * v)))


def peer(n, at, r):
    upper = (2 * at) // n
    down = n - 1 - r
    return upper * (r + (r + n - at) // n) + (1 - upper) * (down - (at + n - down) // n)


def rank(n, at, other):
    upper = (2 * at) // n
    above = (other + n - 1 - at) // n
    below = (at + n - 1 - other) // n
    return upper * (other - above) + (1 - upper) * (n - 1 - other - below)


def kernel(
    n_e,
    n_s,
    tokens_h,
    picks_h,
    gates_h,
    counts_h,
    norm_in_h,
    norm_out_h,
    w_in_h,
    w_out_h,
    w_key_h,
    w_value_h,
    queries_h,
    w_proj_h,
    enc_v,
    dec_v,
    tokens_v,
    picks_v,
    gates_v,
    counts_v,
    norm_in_v,
    norm_out_v,
    w_in_v,
    w_out_v,
    w_key_v,
    w_value_v,
    w_proj_v,
    q_v,
    send_a,
    recv_a,
    send_b,
    recv_b,
    part_v,
    part_r,
    stat_v,
    stat_r,
    load_sem,
    a_send,
    a_recv,
    b_send,
    b_recv,
    q_send,
    q_recv,
    p_send,
    p_recv,
    t_send,
    t_recv,
):
    me_e = lax.axis_index("expert")
    me_s = lax.axis_index("seq")
    helper = lax.rem(me_s, 2)
    rows, width = tokens_v.shape
    slots = send_a.shape[1]
    dec_rows = q_v.shape[1]
    q_width = q_v.shape[2]
    head = q_width // HEADS
    own, far, extra = n_e - 2, n_e - 1, n_e

    loads = {}
    for i, (name, src, dst) in enumerate(
        (
            ("tokens", tokens_h, tokens_v),
            ("norm_in", norm_in_h, norm_in_v),
            ("picks", picks_h, picks_v),
            ("queries", queries_h, q_v.at[me_s]),
            ("w_in", w_in_h.at[0], w_in_v),
            ("w_out", w_out_h.at[0], w_out_v),
            ("gates", gates_h, gates_v),
            ("counts", counts_h, counts_v),
            ("norm_out", norm_out_h, norm_out_v),
            ("w_key", w_key_h, w_key_v),
            ("w_value", w_value_h, w_value_v),
            ("w_proj", w_proj_h, w_proj_v),
        )
    ):
        loads[name] = pltpu.make_async_copy(src, dst, load_sem.at[i])
    loads["tokens"].start()

    barrier = pltpu.get_barrier_semaphore()

    def greet(e, s):
        pl.semaphore_signal(
            barrier, inc=1, device_id={"expert": e, "seq": s}, device_id_type=MESH
        )

    @pl.when(helper == 1)
    def _():
        greet(peer(n_e, me_e, 0), me_s - 1)
        greet(peer(n_e, me_e, 0), me_s)

    for r in range(1, n_e - 1):
        greet(peer(n_e, me_e, r), me_s)
    for d in range(1, n_s):
        greet(me_e, lax.rem(me_s + d, n_s))
    for name in loads:
        if name != "tokens":
            loads[name].start()

    def copy_a(r):
        to = peer(n_e, me_e, r)
        place = rank(n_e, to, me_e)
        first = (n_e - place) // n_e
        aside = first * (1 - helper)
        slot = (1 - first) * (place - 1) + first * far + aside
        return pltpu.make_async_remote_copy(
            src_ref=send_a.at[to],
            dst_ref=recv_a.at[slot],
            send_sem=a_send.at[r],
            recv_sem=a_recv.at[slot],
            device_id={"expert": to, "seq": me_s + aside},
            device_id_type=MESH,
        )

    def arrive_a(slot):
        pltpu.make_async_remote_copy(
            src_ref=send_a.at[0],
            dst_ref=recv_a.at[slot],
            send_sem=a_send.at[0],
            recv_sem=a_recv.at[slot],
            device_id={"expert": peer(n_e, me_e, 0), "seq": me_s},
            device_id_type=MESH,
        ).wait_recv()

    def copy_b(slot):
        r = 0 if slot >= far else slot + 1
        aside = 1 if slot == extra else 0
        return pltpu.make_async_remote_copy(
            src_ref=send_b.at[slot],
            dst_ref=recv_b.at[me_e],
            send_sem=b_send.at[slot],
            recv_sem=b_recv.at[me_e],
            device_id={"expert": peer(n_e, me_e, r), "seq": me_s - aside},
            device_id_type=MESH,
        )

    def arrive_b(r):
        at = peer(n_e, me_e, r)
        pltpu.make_async_remote_copy(
            src_ref=send_b.at[0],
            dst_ref=recv_b.at[at],
            send_sem=b_send.at[0],
            recv_sem=b_recv.at[at],
            device_id={"expert": at, "seq": me_s},
            device_id_type=MESH,
        ).wait_recv()

    def copy_q(d, arriving=False):
        at = lax.rem(me_s + n_s - d, n_s) if arriving else me_s
        return pltpu.make_async_remote_copy(
            src_ref=q_v.at[me_s],
            dst_ref=q_v.at[at],
            send_sem=q_send.at[d],
            recv_sem=q_recv.at[d],
            device_id={"expert": me_e, "seq": lax.rem(me_s + d, n_s)},
            device_id_type=MESH,
        )

    def copy_p(d):
        to = lax.rem(me_s + d, n_s)
        return pltpu.make_async_remote_copy(
            src_ref=part_v.at[to],
            dst_ref=part_r.at[d],
            send_sem=p_send.at[d],
            recv_sem=p_recv.at[d],
            device_id={"expert": me_e, "seq": to},
            device_id_type=MESH,
        )

    def copy_t(d):
        to = lax.rem(me_s + d, n_s)
        return pltpu.make_async_remote_copy(
            src_ref=stat_v.at[to],
            dst_ref=stat_r.at[d],
            send_sem=t_send.at[d],
            recv_sem=t_recv.at[d],
            device_id={"expert": me_e, "seq": to},
            device_id_type=MESH,
        )

    loads["tokens"].wait()
    loads["norm_in"].wait()
    loads["picks"].wait()
    normed = rms_norm(tokens_v[...].astype(F32), norm_in_v[...]).astype(BF16)
    pick_row = jnp.concatenate([picks_v[0, j : j + 1, :] for j in range(n_e)], axis=1)
    position = lax.broadcasted_iota(jnp.int32, (rows, n_e * slots), 0)
    chosen = jnp.where(position == pick_row, 1.0, 0.0).astype(BF16)
    send_a[...] = (
        lax.dot_general(chosen, normed, (((0,), (0,)), ((), ())), preferred_element_type=F32)
        .astype(BF16)
        .reshape(n_e, slots, width)
    )
    pl.semaphore_wait(barrier, n_e - 1 + n_s - 1)
    for r in range(n_e - 1):
        copy_a(r).start()
    loads["queries"].wait()
    for d in range(1, n_s):
        copy_q(d).start()
    recv_a[own] = send_a[me_e]

    loads["gates"].wait()
    loads["counts"].wait()
    slot_lane = lax.broadcasted_iota(jnp.int32, (1, slots), 1)
    gate_row = jnp.concatenate(
        [
            jnp.where(slot_lane < counts_v[0:1, j : j + 1], gates_v[0, j : j + 1, :], 0.0)
            for j in range(n_e)
        ],
        axis=1,
    )
    high = gate_row.astype(BF16).astype(F32)
    middle = (gate_row - high).astype(BF16).astype(F32)
    low = gate_row - high - middle
    gate_three = jnp.concatenate([high, middle, low], axis=1)
    pick_three = jnp.concatenate([pick_row] * 3, axis=1)
    position_three = lax.broadcasted_iota(jnp.int32, (rows, 3 * n_e * slots), 0)
    combine = jnp.where(position_three == pick_three, gate_three, 0.0).astype(BF16)

    def feed(first, many):
        flat = recv_a[first : first + many].reshape(many * slots, width)
        hidden = gelu(jnp.dot(flat, w_in_v[...], preferred_element_type=F32)).astype(BF16)
        result = jnp.dot(hidden, w_out_v[...], preferred_element_type=F32).astype(BF16)
        send_b[first : first + many] = result.reshape(many, slots, width)

    loads["w_in"].wait()
    loads["w_out"].wait()
    for slot in range(own):
        arrive_a(slot)
    feed(0, own + 1)
    for slot in range(own):
        copy_b(slot).start()
    recv_b[me_e] = send_b[own]

    @pl.when(helper == 1)
    def _():
        arrive_a(far)
        arrive_a(extra)
        feed(far, 2)
        copy_b(extra).start()
        copy_b(far).start()

    loads["norm_out"].wait()
    loads["w_key"].wait()
    loads["w_value"].wait()
    for d in range(1, n_s):
        copy_q(d, True).wait_recv()
    all_rows = n_s * dec_rows
    queries = q_v[...].reshape(all_rows, q_width)
    for r in range(n_e - 1):
        arrive_b(n_e - 2 - r)
    returned = recv_b[...].reshape(n_e * slots, width)
    expert_sum = jnp.dot(
        combine, jnp.concatenate([returned] * 3, axis=0), preferred_element_type=F32
    )
    mixed = tokens_v[...].astype(F32) + expert_sum
    encoded = rms_norm(mixed, norm_out_v[...]).astype(BF16)
    enc_v[...] = encoded
    keys = jnp.dot(encoded, w_key_v[...], preferred_element_type=F32).astype(BF16)
    values = jnp.dot(encoded, w_value_v[...], preferred_element_type=F32).astype(BF16)

    slab = min(256, q_width)
    groups = q_width // slab
    group = slab // head
    lanes = stat_v.shape[2]
    lane_head = lax.broadcasted_iota(jnp.int32, (1, slab), 1) // head
    stat_lane = lax.broadcasted_iota(jnp.int32, (1, lanes), 1)
    bands = dec_rows // 8
    tops, totals = [], []
    for g in range(groups):
        cols = slice(g * slab, (g + 1) * slab)
        only = [jnp.where(lane_head == h, 1.0, 0.0).astype(BF16) for h in range(group)]
        key_heads = jnp.concatenate([keys[:, cols] * m for m in only], axis=0)
        value_heads = jnp.concatenate([values[:, cols] * m for m in only], axis=0)
        scores = lax.dot_general(
            queries[:, cols], key_heads, (((1,), (1,)), ((), ())), preferred_element_type=F32
        ) * (head**-0.5)
        weights = []
        for h in range(group):
            span = scores[:, h * rows : (h + 1) * rows]
            row_max = jnp.max(span, axis=1, keepdims=True)
            weight = jnp.exp(span - row_max)
            tops.append(row_max)
            totals.append(jnp.sum(weight, axis=1, keepdims=True))
            weights.append(weight.astype(BF16))
        product = jnp.dot(
            jnp.concatenate(weights, axis=1), value_heads, preferred_element_type=F32
        )
        part_v[:, :, cols] = product.astype(BF16).reshape(n_s, dec_rows, slab)
    for s in range(n_s):
        packed = jnp.zeros((8, lanes), F32)
        for band in range(bands):
            at = s * dec_rows + band * 8
            piece = jnp.zeros((8, lanes), F32)
            for h in range(HEADS):
                lane = band * 2 * HEADS + h
                piece = jnp.where(stat_lane == lane, tops[h][at : at + 8], piece)
                piece = jnp.where(stat_lane == lane + HEADS, totals[h][at : at + 8], piece)
            packed = packed + piece
        stat_v[s] = packed
    for d in range(1, n_s):
        copy_t(d).start()
        copy_p(d).start()
    part_r[0] = part_v[me_s]
    stat_r[0] = stat_v[me_s]

    loads["w_proj"].wait()
    for d in range(1, n_s):
        copy_t(d).wait_recv()
    stat = []
    for d in range(n_s):
        packed = stat_r[d]
        stat.append(
            jnp.concatenate(
                [
                    pltpu.roll(packed, lanes - band * 2 * HEADS, 1) if band else packed
                    for band in range(bands)
                ],
                axis=0,
            )
        )
    top = functools.reduce(jnp.maximum, stat)
    factor = [jnp.exp(s - top)[:, :HEADS] for s in stat]
    total = sum(f * s[:, HEADS : 2 * HEADS] for f, s in zip(factor, stat))
    for d in range(1, n_s):
        copy_p(d).wait_recv()
    answer = None
    for g in range(groups):
        cols = slice(g * slab, (g + 1) * slab)
        summed = jnp.zeros((dec_rows, slab), F32)
        for d in range(n_s):
            scale = factor[d] / total
            at = g * group
            spread = jnp.broadcast_to(scale[:, at : at + 1], (dec_rows, slab))
            for h in range(1, group):
                spread = jnp.where(lane_head == h, scale[:, at + h : at + h + 1], spread)
            summed = summed + spread * part_r[d, :, cols].astype(F32)
        term = jnp.dot(summed.astype(BF16), w_proj_v[cols], preferred_element_type=F32)
        answer = term if answer is None else answer + term
    dec_v[...] = answer.astype(BF16)

    for r in range(n_e - 1):
        copy_a(r).wait_send()
    for slot in range(own):
        copy_b(slot).wait_send()

    @pl.when(helper == 1)
    def _():
        copy_b(extra).wait_send()
        copy_b(far).wait_send()

    for d in range(1, n_s):
        copy_q(d).wait_send()
        copy_p(d).wait_send()
        copy_t(d).wait_send()


def finish(enc_v, dec_v, encoded_h, dec_h, store_sem):
    enc_store = pltpu.make_async_copy(enc_v, encoded_h, store_sem.at[0])
    dec_store = pltpu.make_async_copy(dec_v, dec_h, store_sem.at[1])
    enc_store.start()
    dec_store.start()
    enc_store.wait()
    dec_store.wait()


def local(
    n_e,
    n_s,
    tokens,
    picks,
    gates,
    counts,
    norm_in,
    norm_out,
    w_in,
    w_out,
    w_key,
    w_value,
    queries,
    w_proj,
):
    rows, width = tokens.shape
    slots = picks.shape[2]
    hidden = w_in.shape[2]
    dec_rows, q_width = queries.shape
    lanes = 128 * pl.cdiv((dec_rows // 8) * 2 * HEADS, 128)
    anywhere = pl.BlockSpec(memory_space=pl.ANY)
    dma = pltpu.SemaphoreType.DMA
    vmem = pl.BlockSpec(memory_space=pltpu.VMEM)
    room = 2 * (rows * width + dec_rows * width)
    encoded, dec = pl.pallas_call(
        functools.partial(kernel, n_e, n_s),
        out_shape=(
            pltpu.VMEM((rows, width), BF16),
            pltpu.VMEM((dec_rows, width), BF16),
        ),
        in_specs=[anywhere] * 12,
        out_specs=(vmem, vmem),
        scratch_shapes=[
            pltpu.VMEM((rows, width), BF16),
            pltpu.VMEM(picks.shape, jnp.int32),
            pltpu.VMEM(gates.shape, F32),
            pltpu.VMEM(counts.shape, jnp.int32),
            pltpu.VMEM((1, width), F32),
            pltpu.VMEM((1, width), F32),
            pltpu.VMEM((width, hidden), BF16),
            pltpu.VMEM((hidden, width), BF16),
            pltpu.VMEM((width, q_width), BF16),
            pltpu.VMEM((width, q_width), BF16),
            pltpu.VMEM((q_width, width), BF16),
            pltpu.VMEM((n_s, dec_rows, q_width), BF16),
            pltpu.VMEM((n_e, slots, width), BF16),
            pltpu.VMEM((n_e + 1, slots, width), BF16),
            pltpu.VMEM((n_e + 1, slots, width), BF16),
            pltpu.VMEM((n_e, slots, width), BF16),
            pltpu.VMEM((n_s, dec_rows, q_width), BF16),
            pltpu.VMEM((n_s, dec_rows, q_width), BF16),
            pltpu.VMEM((n_s, 8, lanes), F32),
            pltpu.VMEM((n_s, 8, lanes), F32),
            dma((12,)),
            dma((n_e - 1,)),
            dma((n_e + 1,)),
            dma((n_e + 1,)),
            dma((n_e,)),
            dma((n_s,)),
            dma((n_s,)),
            dma((n_s,)),
            dma((n_s,)),
            dma((n_s,)),
            dma((n_s,)),
        ],
        compiler_params=pltpu.CompilerParams(
            collective_id=0, has_side_effects=True, vmem_limit_bytes=VMEM_BYTES - room
        ),
    )(
        tokens,
        picks,
        gates,
        counts,
        norm_in.reshape(1, -1),
        norm_out.reshape(1, -1),
        w_in,
        w_out,
        w_key,
        w_value,
        queries,
        w_proj,
    )
    return pl.pallas_call(
        finish,
        out_shape=(
            jax.ShapeDtypeStruct((rows, width), BF16),
            jax.ShapeDtypeStruct((dec_rows, width), BF16),
        ),
        in_specs=[vmem] * 2,
        out_specs=(anywhere, anywhere),
        scratch_shapes=[dma((2,))],
        compiler_params=pltpu.CompilerParams(vmem_limit_bytes=8 * 2**20),
    )(encoded, dec)


def solution(mesh):
    in_specs = (
        P(("dp", "expert", "seq"), None),
        P(("dp", "expert", "seq"), None, None),
        P(("dp", "expert", "seq"), None, None),
        P(("dp", "expert", "seq"), None),
        P(),
        P(),
        P("expert", None, None),
        P("expert", None, None),
        P(),
        P(),
        P(("dp", "expert", "seq"), None),
        P(),
    )
    out_specs = (P(("dp", "expert", "seq"), None), P(("dp", "expert", "seq"), None))
    body = functools.partial(local, mesh.shape["expert"], mesh.shape["seq"])
    return jax.shard_map(body, mesh=mesh, in_specs=in_specs, out_specs=out_specs, check_vma=False)
```

```python
import functools

import jax
import jax.numpy as jnp
from jax import lax
from jax.experimental import pallas as pl
from jax.experimental.pallas import tpu as pltpu
from jax.sharding import PartitionSpec as P

HEADS = 8
EPSILON = 1e-06
VMEM_BYTES = 67043328
MESH = pl.DeviceIdType.MESH
F32 = jnp.float32
BF16 = jnp.bfloat16


def rms_norm(values, gain):
    mean_square = jnp.mean(values * values, axis=-1, keepdims=True)
    return values * lax.rsqrt(mean_square + EPSILON) * gain


def gelu(v):
    return 0.5 * v * (1.0 + jnp.tanh(0.7978845608028654 * (v + 0.044715 * v * v * v)))


def peer(n, at, r):
    upper = lax.div(2 * at, n)
    down = n - 1 - r
    return upper * (r + lax.div(r + n - at, n)) + (1 - upper) * (down - lax.div(at + n - down, n))


def rank(n, at, other):
    upper = lax.div(2 * at, n)
    above = lax.div(other + n - 1 - at, n)
    below = lax.div(at + n - 1 - other, n)
    return upper * (other - above) + (1 - upper) * (n - 1 - other - below)


def kernel(
    n_e,
    n_s,
    tokens_h,
    picks_h,
    gates_h,
    counts_h,
    norm_in_h,
    norm_out_h,
    w_in_h,
    w_out_h,
    w_key_h,
    w_value_h,
    queries_h,
    w_proj_h,
    enc_v,
    dec_v,
    tokens_v,
    picks_v,
    gates_v,
    counts_v,
    norms_v,
    w_in_v,
    w_out_v,
    w_kv_v,
    w_proj_v,
    q_v,
    send_a,
    recv_a,
    send_b,
    recv_b,
    part_v,
    part_r,
    stat_v,
    stat_r,
    spread_v,
    load_sem,
    a_send,
    a_recv,
    b_send,
    b_recv,
    q_send,
    q_recv,
    p_send,
    p_recv,
    t_send,
    t_recv,
):
    me_e = lax.axis_index("expert")
    me_s = lax.axis_index("seq")
    helper = lax.rem(me_s, 2)
    rows, width = tokens_v.shape
    slots = send_a.shape[1]
    dec_rows = q_v.shape[1]
    q_width = q_v.shape[2]
    head = q_width // HEADS
    own, far, extra = n_e - 2, n_e - 1, n_e

    loads = {}
    for i, (name, src, dst) in enumerate(
        (
            ("tokens", tokens_h, tokens_v),
            ("picks", picks_h, picks_v),
            ("queries", queries_h, q_v.at[me_s]),
            ("w_in", w_in_h.at[0], w_in_v),
            ("w_out", w_out_h.at[0], w_out_v),
            ("gates", gates_h, gates_v),
            ("counts", counts_h, counts_v),
            ("w_proj", w_proj_h, w_proj_v),
        )
    ):
        loads[name] = pltpu.make_async_copy(src, dst, load_sem.at[i])
    pairs = {}
    for i, (name, parts, dst) in enumerate(
        (("norms", (norm_in_h, norm_out_h), norms_v), ("w_kv", (w_key_h, w_value_h), w_kv_v))
    ):
        sem = load_sem.at[len(loads) + i]
        pairs[name] = [
            pltpu.make_async_copy(part, dst.at[k], sem) for k, part in enumerate(parts)
        ]
    both = {
        name: pltpu.make_async_copy(dst, dst, load_sem.at[len(loads) + i])
        for i, (name, dst) in enumerate((("norms", norms_v), ("w_kv", w_kv_v)))
    }
    loads["tokens"].start()
    loads["picks"].start()
    for copy in pairs["norms"]:
        copy.start()

    barrier = pltpu.get_barrier_semaphore()

    def greet(e, s):
        pl.semaphore_signal(
            barrier, inc=1, device_id={"expert": e, "seq": s}, device_id_type=MESH
        )

    @pl.when(helper == 1)
    def _():
        greet(peer(n_e, me_e, 0), me_s - 1)
        greet(peer(n_e, me_e, 0), me_s)

    for r in range(1, n_e - 1):
        greet(peer(n_e, me_e, r), me_s)
    for d in range(1, n_s):
        greet(me_e, lax.rem(me_s + d, n_s))
    for name in ("queries", "w_in", "w_out", "gates", "counts"):
        loads[name].start()
    for copy in pairs["w_kv"]:
        copy.start()
    loads["w_proj"].start()

    def remote(src, dst, send, recv, e, s):
        return pltpu.make_async_remote_copy(
            src_ref=src,
            dst_ref=dst,
            send_sem=send,
            recv_sem=recv,
            device_id={"expert": e, "seq": s},
            device_id_type=MESH,
        )

    def copy_a(r):
        to = peer(n_e, me_e, r)
        place = rank(n_e, to, me_e)
        first = lax.div(n_e - place, n_e)
        aside = first * (1 - helper)
        slot = (1 - first) * (place - 1) + first * far + aside
        return remote(
            send_a.at[to], recv_a.at[slot], a_send.at[0], a_recv.at[first + aside], to, me_s + aside
        )

    def copy_b(slot):
        aside = 1 if slot == extra else 0
        return remote(
            send_b.at[slot],
            recv_b.at[me_e],
            b_send.at[1 if slot >= far else 0],
            b_recv.at[0],
            peer(n_e, me_e, 0 if slot >= far else slot + 1),
            me_s - aside,
        )

    def whole(ref, first, many, sem):
        piece = ref.at[pl.ds(first, many)]
        return pltpu.make_async_copy(piece, piece, sem)

    def copy_q(d):
        to = lax.rem(me_s + d, n_s)
        return remote(q_v.at[me_s], q_v.at[me_s], q_send.at[0], q_recv.at[0], me_e, to)

    def copy_p(d):
        to = lax.rem(me_s + d, n_s)
        return remote(part_v.at[to], part_r.at[d], p_send.at[0], p_recv.at[0], me_e, to)

    def copy_t(d):
        to = lax.rem(me_s + d, n_s)
        return remote(stat_v.at[to], stat_r.at[d], t_send.at[0], t_recv.at[0], me_e, to)

    a_copies = [copy_a(r) for r in range(n_e - 1)]
    loads["tokens"].wait()
    both["norms"].wait()
    loads["picks"].wait()
    normed = rms_norm(tokens_v[...].astype(F32), norms_v[0]).astype(BF16)
    pick_row = jnp.concatenate([picks_v[0, j : j + 1, :] for j in range(n_e)], axis=1)
    position = lax.broadcasted_iota(jnp.int32, (rows, n_e * slots), 0)
    chosen = jnp.where(position == pick_row, 1.0, 0.0).astype(BF16)
    send_a[...] = (
        lax.dot_general(chosen, normed, (((0,), (0,)), ((), ())), preferred_element_type=F32)
        .astype(BF16)
        .reshape(n_e, slots, width)
    )
    pl.semaphore_wait(barrier, n_e - 1 + n_s - 1)
    for copy in a_copies:
        copy.start()
    loads["queries"].wait()
    for d in range(1, n_s):
        copy_q(d).start()
    recv_a[own] = send_a[me_e]

    loads["gates"].wait()
    loads["counts"].wait()
    slot_lane = lax.broadcasted_iota(jnp.int32, (1, slots), 1)
    gate_row = jnp.concatenate(
        [
            jnp.where(slot_lane < counts_v[0:1, j : j + 1], gates_v[0, j : j + 1, :], 0.0)
            for j in range(n_e)
        ],
        axis=1,
    )
    high = gate_row.astype(BF16).astype(F32)
    middle = (gate_row - high).astype(BF16).astype(F32)
    low = gate_row - high - middle
    gate_three = jnp.concatenate([high, middle, low], axis=1)
    pick_three = jnp.concatenate([pick_row] * 3, axis=1)
    position_three = lax.broadcasted_iota(jnp.int32, (rows, 3 * n_e * slots), 0)
    combine = jnp.where(position_three == pick_three, gate_three, 0.0).astype(BF16)

    def feed(first, many):
        flat = recv_a[first : first + many].reshape(many * slots, width)
        hidden = gelu(jnp.dot(flat, w_in_v[...], preferred_element_type=F32)).astype(BF16)
        result = jnp.dot(hidden, w_out_v[...], preferred_element_type=F32).astype(BF16)
        send_b[first : first + many] = result.reshape(many, slots, width)

    loads["w_in"].wait()
    loads["w_out"].wait()
    feed(own, 1)
    recv_b[me_e] = send_b[own]
    whole(recv_a, 0, own, a_recv.at[0]).wait()
    feed(0, own)
    for slot in range(own):
        copy_b(slot).start()

    @pl.when(helper == 1)
    def _():
        whole(recv_a, far, 1, a_recv.at[1]).wait()
        feed(far, 1)
        copy_b(far).start()
        whole(recv_a, extra, 1, a_recv.at[2]).wait()
        feed(extra, 1)
        copy_b(extra).start()

    both["w_kv"].wait()
    whole(q_v, 0, n_s - 1, q_recv.at[0]).wait()
    all_rows = n_s * dec_rows
    queries = q_v[...].reshape(all_rows, q_width)
    whole(recv_b, 0, n_e - 1, b_recv.at[0]).wait()
    returned = recv_b[...].reshape(n_e * slots, width)
    expert_sum = jnp.dot(
        combine, jnp.concatenate([returned] * 3, axis=0), preferred_element_type=F32
    )
    mixed = tokens_v[...].astype(F32) + expert_sum
    encoded = rms_norm(mixed, norms_v[1]).astype(BF16)
    enc_v[...] = encoded
    slab = min(256, q_width)
    groups = q_width // slab
    group = slab // head
    lanes = stat_v.shape[2]
    lane_head = lax.broadcasted_iota(jnp.int32, (1, slab), 1) // head
    stat_lane = lax.broadcasted_iota(jnp.int32, (1, lanes), 1)
    bands = dec_rows // 8
    only = [jnp.where(lane_head == h, 1.0, 0.0).astype(BF16) for h in range(group)]
    slabs = [slice(g * slab, (g + 1) * slab) for g in range(groups)]
    keys = jnp.dot(encoded, w_kv_v[0], preferred_element_type=F32).astype(BF16)
    scores = []
    for cols in slabs:
        key_heads = jnp.concatenate([keys[:, cols] * m for m in only], axis=0)
        scores.append(
            lax.dot_general(
                queries[:, cols], key_heads, (((1,), (1,)), ((), ())), preferred_element_type=F32
            )
            * (head**-0.5)
        )
    values = jnp.dot(encoded, w_kv_v[1], preferred_element_type=F32).astype(BF16)
    tops, totals = [], []
    for cols, score in zip(slabs, scores):
        weights = []
        for h in range(group):
            span = score[:, h * rows : (h + 1) * rows]
            row_max = jnp.max(span, axis=1, keepdims=True)
            weight = jnp.exp(span - row_max)
            tops.append(row_max)
            totals.append(jnp.sum(weight, axis=1, keepdims=True))
            weights.append(weight.astype(BF16))
        value_heads = jnp.concatenate([values[:, cols] * m for m in only], axis=0)
        product = jnp.dot(
            jnp.concatenate(weights, axis=1), value_heads, preferred_element_type=F32
        )
        part_v[:, :, cols] = product.astype(BF16).reshape(n_s, dec_rows, slab)
    for s in range(n_s):
        packed = jnp.zeros((8, lanes), F32)
        for band in range(bands):
            at = s * dec_rows + band * 8
            piece = jnp.zeros((8, lanes), F32)
            for h in range(HEADS):
                lane = band * 2 * HEADS + h
                piece = jnp.where(stat_lane == lane, tops[h][at : at + 8], piece)
                piece = jnp.where(stat_lane == lane + HEADS, totals[h][at : at + 8], piece)
            packed = packed + piece
        stat_v[s] = packed
    for d in range(1, n_s):
        copy_t(d).start()
        copy_p(d).start()
    part_r[0] = part_v[me_s]
    stat_r[0] = stat_v[me_s]

    whole(send_a, 0, n_e - 1, a_send.at[0]).wait()
    whole(send_b, 0, own, b_send.at[0]).wait()

    @pl.when(helper == 1)
    def _():
        whole(send_b, far, 2, b_send.at[1]).wait()

    whole(q_v, 0, n_s - 1, q_send.at[0]).wait()
    loads["w_proj"].wait()
    whole(stat_r, 1, n_s - 1, t_recv.at[0]).wait()
    stat = []
    for d in range(n_s):
        packed = stat_r[d]
        stat.append(
            jnp.concatenate(
                [
                    pltpu.roll(packed, lanes - band * 2 * HEADS, 1) if band else packed
                    for band in range(bands)
                ],
                axis=0,
            )
        )
    top = functools.reduce(jnp.maximum, stat)
    factor = [jnp.exp(s - top)[:, :HEADS] for s in stat]
    total = sum(f * s[:, HEADS : 2 * HEADS] for f, s in zip(factor, stat))
    for d in range(n_s):
        scale = factor[d] / total
        for g, cols in enumerate(slabs):
            at = g * group
            spread = jnp.broadcast_to(scale[:, at : at + 1], (dec_rows, slab))
            for h in range(1, group):
                spread = jnp.where(lane_head == h, scale[:, at + h : at + h + 1], spread)
            spread_v[d, :, cols] = spread
    whole(stat_v, 0, n_s - 1, t_send.at[0]).wait()
    whole(part_v, 0, n_s - 1, p_send.at[0]).wait()
    whole(part_r, 1, n_s - 1, p_recv.at[0]).wait()
    summed = sum(spread_v[d] * part_r[d].astype(F32) for d in range(n_s))
    dec_v[...] = jnp.dot(
        summed.astype(BF16), w_proj_v[...], preferred_element_type=F32
    ).astype(BF16)


def finish(enc_v, dec_v, encoded_h, dec_h, store_sem):
    enc_store = pltpu.make_async_copy(enc_v, encoded_h, store_sem.at[0])
    dec_store = pltpu.make_async_copy(dec_v, dec_h, store_sem.at[1])
    enc_store.start()
    dec_store.start()
    enc_store.wait()
    dec_store.wait()


def local(
    n_e,
    n_s,
    tokens,
    picks,
    gates,
    counts,
    norm_in,
    norm_out,
    w_in,
    w_out,
    w_key,
    w_value,
    queries,
    w_proj,
):
    rows, width = tokens.shape
    slots = picks.shape[2]
    hidden = w_in.shape[2]
    dec_rows, q_width = queries.shape
    lanes = 128 * pl.cdiv((dec_rows // 8) * 2 * HEADS, 128)
    anywhere = pl.BlockSpec(memory_space=pl.ANY)
    dma = pltpu.SemaphoreType.DMA
    vmem = pl.BlockSpec(memory_space=pltpu.VMEM)
    room = 2 * (rows * width + dec_rows * width)
    encoded, dec = pl.pallas_call(
        functools.partial(kernel, n_e, n_s),
        out_shape=(
            pltpu.VMEM((rows, width), BF16),
            pltpu.VMEM((dec_rows, width), BF16),
        ),
        in_specs=[anywhere] * 12,
        out_specs=(vmem, vmem),
        scratch_shapes=[
            pltpu.VMEM((rows, width), BF16),
            pltpu.VMEM(picks.shape, jnp.int32),
            pltpu.VMEM(gates.shape, F32),
            pltpu.VMEM(counts.shape, jnp.int32),
            pltpu.VMEM((2, 1, width), F32),
            pltpu.VMEM((width, hidden), BF16),
            pltpu.VMEM((hidden, width), BF16),
            pltpu.VMEM((2, width, q_width), BF16),
            pltpu.VMEM((q_width, width), BF16),
            pltpu.VMEM((n_s, dec_rows, q_width), BF16),
            pltpu.VMEM((n_e, slots, width), BF16),
            pltpu.VMEM((n_e + 1, slots, width), BF16),
            pltpu.VMEM((n_e + 1, slots, width), BF16),
            pltpu.VMEM((n_e, slots, width), BF16),
            pltpu.VMEM((n_s, dec_rows, q_width), BF16),
            pltpu.VMEM((n_s, dec_rows, q_width), BF16),
            pltpu.VMEM((n_s, 8, lanes), F32),
            pltpu.VMEM((n_s, 8, lanes), F32),
            pltpu.VMEM((n_s, dec_rows, q_width), F32),
            dma((10,)),
            dma((1,)),
            dma((3,)),
            dma((2,)),
            dma((1,)),
            dma((1,)),
            dma((1,)),
            dma((1,)),
            dma((1,)),
            dma((1,)),
            dma((1,)),
        ],
        compiler_params=pltpu.CompilerParams(
            collective_id=0, has_side_effects=True, vmem_limit_bytes=VMEM_BYTES - room
        ),
    )(
        tokens,
        picks,
        gates,
        counts,
        norm_in.reshape(1, -1),
        norm_out.reshape(1, -1),
        w_in,
        w_out,
        w_key,
        w_value,
        queries,
        w_proj,
    )
    return pl.pallas_call(
        finish,
        out_shape=(
            jax.ShapeDtypeStruct((rows, width), BF16),
            jax.ShapeDtypeStruct((dec_rows, width), BF16),
        ),
        in_specs=[vmem] * 2,
        out_specs=(anywhere, anywhere),
        scratch_shapes=[dma((2,))],
        compiler_params=pltpu.CompilerParams(vmem_limit_bytes=8 * 2**20),
    )(encoded, dec)


def solution(mesh):
    in_specs = (
        P(("dp", "expert", "seq"), None),
        P(("dp", "expert", "seq"), None, None),
        P(("dp", "expert", "seq"), None, None),
        P(("dp", "expert", "seq"), None),
        P(),
        P(),
        P("expert", None, None),
        P("expert", None, None),
        P(),
        P(),
        P(("dp", "expert", "seq"), None),
        P(),
    )
    out_specs = (P(("dp", "expert", "seq"), None), P(("dp", "expert", "seq"), None))
    body = functools.partial(local, mesh.shape["expert"], mesh.shape["seq"])
    return jax.shard_map(body, mesh=mesh, in_specs=in_specs, out_specs=out_specs, check_vma=False)
```

```python
import functools

import jax
import jax.numpy as jnp
from jax import lax
from jax.experimental import pallas as pl
from jax.experimental.pallas import tpu as pltpu
from jax.sharding import PartitionSpec as P

HEADS = 8
EPSILON = 1e-06
VMEM_BYTES = 67043328
MESH = pl.DeviceIdType.MESH
F32 = jnp.float32
BF16 = jnp.bfloat16


def rms_norm(values, gain):
    mean_square = jnp.mean(values * values, axis=-1, keepdims=True)
    return values * lax.rsqrt(mean_square + EPSILON) * gain


def gelu(v):
    return 0.5 * v * (1.0 + jnp.tanh(0.7978845608028654 * (v + 0.044715 * v * v * v)))


def peer(n, at, r):
    upper = lax.div(2 * at, n)
    down = n - 1 - r
    return upper * (r + lax.div(r + n - at, n)) + (1 - upper) * (down - lax.div(at + n - down, n))


def rank(n, at, other):
    upper = lax.div(2 * at, n)
    above = lax.div(other + n - 1 - at, n)
    below = lax.div(at + n - 1 - other, n)
    return upper * (other - above) + (1 - upper) * (n - 1 - other - below)


def kernel(
    n_e,
    n_s,
    tokens_h,
    picks_h,
    gates_h,
    counts_h,
    norm_in_h,
    norm_out_h,
    w_in_h,
    w_out_h,
    w_key_h,
    w_value_h,
    queries_h,
    w_proj_h,
    enc_v,
    dec_v,
    tokens_v,
    picks_v,
    gates_v,
    counts_v,
    norms_v,
    w_in_v,
    w_out_v,
    w_kv_v,
    w_proj_v,
    q_v,
    send_a,
    recv_a,
    send_b,
    recv_b,
    part_v,
    part_r,
    stat_v,
    stat_r,
    spread_v,
    load_sem,
    a_send,
    a_recv,
    b_send,
    b_recv,
    q_send,
    q_recv,
    p_send,
    p_recv,
    t_send,
    t_recv,
):
    me_e = lax.axis_index("expert")
    me_s = lax.axis_index("seq")
    helper = lax.rem(me_s, 2)
    rows, width = tokens_v.shape
    slots = send_a.shape[1]
    dec_rows = q_v.shape[1]
    q_width = q_v.shape[2]
    head = q_width // HEADS
    own, far, extra = n_e - 2, n_e - 1, n_e

    loads = {}
    for i, (name, src, dst) in enumerate(
        (
            ("tokens", tokens_h, tokens_v),
            ("picks", picks_h, picks_v),
            ("queries", queries_h, q_v.at[me_s]),
            ("w_in", w_in_h.at[0], w_in_v),
            ("w_out", w_out_h.at[0], w_out_v),
            ("gates", gates_h, gates_v),
            ("counts", counts_h, counts_v),
            ("w_proj", w_proj_h, w_proj_v),
        )
    ):
        loads[name] = pltpu.make_async_copy(src, dst, load_sem.at[i])
    pairs = {}
    for i, (name, parts, dst) in enumerate(
        (("norms", (norm_in_h, norm_out_h), norms_v), ("w_kv", (w_key_h, w_value_h), w_kv_v))
    ):
        sem = load_sem.at[len(loads) + i]
        pairs[name] = [
            pltpu.make_async_copy(part, dst.at[k], sem) for k, part in enumerate(parts)
        ]
    both = {
        name: pltpu.make_async_copy(dst, dst, load_sem.at[len(loads) + i])
        for i, (name, dst) in enumerate((("norms", norms_v), ("w_kv", w_kv_v)))
    }
    loads["tokens"].start()
    loads["picks"].start()
    for copy in pairs["norms"]:
        copy.start()

    barrier = pltpu.get_barrier_semaphore()

    def greet(e, s):
        pl.semaphore_signal(
            barrier, inc=1, device_id={"expert": e, "seq": s}, device_id_type=MESH
        )

    @pl.when(helper == 1)
    def _():
        greet(peer(n_e, me_e, 0), me_s - 1)
        greet(peer(n_e, me_e, 0), me_s)

    for r in range(1, n_e - 1):
        greet(peer(n_e, me_e, r), me_s)
    for d in range(1, n_s):
        greet(me_e, lax.rem(me_s + d, n_s))
    for name in ("queries", "w_in", "w_out", "gates", "counts"):
        loads[name].start()
    for copy in pairs["w_kv"]:
        copy.start()
    loads["w_proj"].start()

    def remote(src, dst, send, recv, e, s):
        return pltpu.make_async_remote_copy(
            src_ref=src,
            dst_ref=dst,
            send_sem=send,
            recv_sem=recv,
            device_id={"expert": e, "seq": s},
            device_id_type=MESH,
        )

    def copy_a(r):
        to = peer(n_e, me_e, r)
        place = rank(n_e, to, me_e)
        first = lax.div(n_e - place, n_e)
        aside = first * (1 - helper)
        slot = (1 - first) * (place - 1) + first * far + aside
        return remote(
            send_a.at[to], recv_a.at[slot], a_send.at[0], a_recv.at[slot], to, me_s + aside
        )

    def copy_b(slot):
        aside = 1 if slot == extra else 0
        return remote(
            send_b.at[slot],
            recv_b.at[me_e],
            b_send.at[1 if slot >= far else 0],
            b_recv.at[0],
            peer(n_e, me_e, 0 if slot >= far else slot + 1),
            me_s - aside,
        )

    def whole(ref, first, many, sem):
        piece = ref.at[pl.ds(first, many)]
        return pltpu.make_async_copy(piece, piece, sem)

    def copy_q(d):
        to = lax.rem(me_s + d, n_s)
        return remote(q_v.at[me_s], q_v.at[me_s], q_send.at[0], q_recv.at[0], me_e, to)

    def copy_p(d):
        to = lax.rem(me_s + d, n_s)
        return remote(part_v.at[to], part_r.at[d], p_send.at[0], p_recv.at[0], me_e, to)

    def copy_t(d):
        to = lax.rem(me_s + d, n_s)
        return remote(stat_v.at[to], stat_r.at[d], t_send.at[0], t_recv.at[0], me_e, to)

    a_copies = [copy_a(r) for r in range(n_e - 1)]
    loads["tokens"].wait()
    both["norms"].wait()
    loads["picks"].wait()
    normed = rms_norm(tokens_v[...].astype(F32), norms_v[0]).astype(BF16)
    pick_row = jnp.concatenate([picks_v[0, j : j + 1, :] for j in range(n_e)], axis=1)
    position = lax.broadcasted_iota(jnp.int32, (rows, n_e * slots), 0)
    chosen = jnp.where(position == pick_row, 1.0, 0.0).astype(BF16)
    send_a[...] = (
        lax.dot_general(chosen, normed, (((0,), (0,)), ((), ())), preferred_element_type=F32)
        .astype(BF16)
        .reshape(n_e, slots, width)
    )
    pl.semaphore_wait(barrier, n_e - 1 + n_s - 1)
    for copy in a_copies:
        copy.start()
    loads["queries"].wait()
    for d in range(1, n_s):
        copy_q(d).start()
    recv_a[own] = send_a[me_e]

    loads["gates"].wait()
    loads["counts"].wait()
    slot_lane = lax.broadcasted_iota(jnp.int32, (1, slots), 1)
    gate_row = jnp.concatenate(
        [
            jnp.where(slot_lane < counts_v[0:1, j : j + 1], gates_v[0, j : j + 1, :], 0.0)
            for j in range(n_e)
        ],
        axis=1,
    )
    high = gate_row.astype(BF16).astype(F32)
    middle = (gate_row - high).astype(BF16).astype(F32)
    low = gate_row - high - middle
    gate_three = jnp.concatenate([high, middle, low], axis=1)
    pick_three = jnp.concatenate([pick_row] * 3, axis=1)
    position_three = lax.broadcasted_iota(jnp.int32, (rows, 3 * n_e * slots), 0)
    combine = jnp.where(position_three == pick_three, gate_three, 0.0).astype(BF16)

    def feed(first, many, second=0, more=0):
        flat = recv_a[first : first + many].reshape(many * slots, width)
        if more:
            rest = recv_a[second : second + more].reshape(more * slots, width)
            flat = jnp.concatenate([flat, rest], axis=0)
        hidden = gelu(jnp.dot(flat, w_in_v[...], preferred_element_type=F32)).astype(BF16)
        result = jnp.dot(hidden, w_out_v[...], preferred_element_type=F32).astype(BF16)
        send_b[first : first + many] = result[: many * slots].reshape(many, slots, width)
        if more:
            send_b[second : second + more] = result[many * slots :].reshape(more, slots, width)

    loads["w_in"].wait()
    loads["w_out"].wait()
    feed(own, 1)
    recv_b[me_e] = send_b[own]
    near = [whole(recv_a, slot, 1, a_recv.at[slot]) for slot in range(own)]
    far_own = whole(recv_a, far, 1, a_recv.at[far])
    far_aside = whole(recv_a, extra, 1, a_recv.at[extra])
    together = helper * lax.div(2 * me_e, n_e) * (1 - lax.div(me_e + 1, n_e))

    @pl.when(together == 1)
    def _():
        for copy in near:
            copy.wait()
        far_own.wait()
        feed(0, own, far, 1)
        copy_b(far).start()
        for slot in range(own):
            copy_b(slot).start()
        far_aside.wait()
        feed(extra, 1)
        copy_b(extra).start()

    @pl.when(helper == 0)
    def _():
        for slot in reversed(range(own)):
            near[slot].wait()
            feed(slot, 1)
            copy_b(slot).start()

    @pl.when(helper - together == 1)
    def _():
        for copy in near:
            copy.wait()
        feed(0, own)
        for slot in range(own):
            copy_b(slot).start()


    @pl.when(helper - together == 1)
    def _():
        far_own.wait()
        feed(far, 1)
        copy_b(far).start()
        far_aside.wait()
        feed(extra, 1)
        copy_b(extra).start()

    both["w_kv"].wait()
    whole(q_v, 0, n_s - 1, q_recv.at[0]).wait()
    all_rows = n_s * dec_rows
    queries = q_v[...].reshape(all_rows, q_width)
    whole(recv_b, 0, n_e - 1, b_recv.at[0]).wait()
    returned = recv_b[...].reshape(n_e * slots, width)
    expert_sum = jnp.dot(
        combine, jnp.concatenate([returned] * 3, axis=0), preferred_element_type=F32
    )
    mixed = tokens_v[...].astype(F32) + expert_sum
    encoded = rms_norm(mixed, norms_v[1]).astype(BF16)
    enc_v[...] = encoded
    slab = min(256, q_width)
    groups = q_width // slab
    group = slab // head
    lanes = stat_v.shape[2]
    lane_head = lax.broadcasted_iota(jnp.int32, (1, slab), 1) // head
    stat_lane = lax.broadcasted_iota(jnp.int32, (1, lanes), 1)
    bands = dec_rows // 8
    only = [jnp.where(lane_head == h, 1.0, 0.0).astype(BF16) for h in range(group)]
    slabs = [slice(g * slab, (g + 1) * slab) for g in range(groups)]
    keys = jnp.dot(encoded, w_kv_v[0], preferred_element_type=F32).astype(BF16)
    scores = []
    for cols in slabs:
        key_heads = jnp.concatenate([keys[:, cols] * m for m in only], axis=0)
        scores.append(
            lax.dot_general(
                queries[:, cols], key_heads, (((1,), (1,)), ((), ())), preferred_element_type=F32
            )
            * (head**-0.5)
        )
    values = jnp.dot(encoded, w_kv_v[1], preferred_element_type=F32).astype(BF16)
    tops, totals = [], []
    for cols, score in zip(slabs, scores):
        weights = []
        for h in range(group):
            span = score[:, h * rows : (h + 1) * rows]
            row_max = jnp.max(span, axis=1, keepdims=True)
            weight = jnp.exp(span - row_max)
            tops.append(row_max)
            totals.append(jnp.sum(weight, axis=1, keepdims=True))
            weights.append(weight.astype(BF16))
        value_heads = jnp.concatenate([values[:, cols] * m for m in only], axis=0)
        product = jnp.dot(
            jnp.concatenate(weights, axis=1), value_heads, preferred_element_type=F32
        )
        part_v[:, :, cols] = product.astype(BF16).reshape(n_s, dec_rows, slab)
    for s in range(n_s):
        packed = jnp.zeros((8, lanes), F32)
        for band in range(bands):
            at = s * dec_rows + band * 8
            piece = jnp.zeros((8, lanes), F32)
            for h in range(HEADS):
                lane = band * 2 * HEADS + h
                piece = jnp.where(stat_lane == lane, tops[h][at : at + 8], piece)
                piece = jnp.where(stat_lane == lane + HEADS, totals[h][at : at + 8], piece)
            packed = packed + piece
        stat_v[s] = packed
    for d in range(1, n_s):
        copy_t(d).start()
        copy_p(d).start()
    part_r[0] = part_v[me_s]
    stat_r[0] = stat_v[me_s]

    whole(send_a, 0, n_e - 1, a_send.at[0]).wait()
    whole(send_b, 0, own, b_send.at[0]).wait()

    @pl.when(helper == 1)
    def _():
        whole(send_b, far, 2, b_send.at[1]).wait()

    whole(q_v, 0, n_s - 1, q_send.at[0]).wait()
    loads["w_proj"].wait()
    whole(stat_r, 1, n_s - 1, t_recv.at[0]).wait()
    stat = []
    for d in range(n_s):
        packed = stat_r[d]
        stat.append(
            jnp.concatenate(
                [
                    pltpu.roll(packed, lanes - band * 2 * HEADS, 1) if band else packed
                    for band in range(bands)
                ],
                axis=0,
            )
        )
    top = functools.reduce(jnp.maximum, stat)
    factor = [jnp.exp(s - top)[:, :HEADS] for s in stat]
    total = sum(f * s[:, HEADS : 2 * HEADS] for f, s in zip(factor, stat))
    for d in range(n_s):
        scale = factor[d] / total
        for g, cols in enumerate(slabs):
            at = g * group
            spread = jnp.broadcast_to(scale[:, at : at + 1], (dec_rows, slab))
            for h in range(1, group):
                spread = jnp.where(lane_head == h, scale[:, at + h : at + h + 1], spread)
            spread_v[d, :, cols] = spread
    whole(stat_v, 0, n_s - 1, t_send.at[0]).wait()
    whole(part_v, 0, n_s - 1, p_send.at[0]).wait()
    whole(part_r, 1, n_s - 1, p_recv.at[0]).wait()
    summed = sum(spread_v[d] * part_r[d].astype(F32) for d in range(n_s))
    dec_v[...] = jnp.dot(
        summed.astype(BF16), w_proj_v[...], preferred_element_type=F32
    ).astype(BF16)


def finish(enc_v, dec_v, encoded_h, dec_h, store_sem):
    enc_store = pltpu.make_async_copy(enc_v, encoded_h, store_sem.at[0])
    dec_store = pltpu.make_async_copy(dec_v, dec_h, store_sem.at[1])
    enc_store.start()
    dec_store.start()
    enc_store.wait()
    dec_store.wait()


def local(
    n_e,
    n_s,
    tokens,
    picks,
    gates,
    counts,
    norm_in,
    norm_out,
    w_in,
    w_out,
    w_key,
    w_value,
    queries,
    w_proj,
):
    rows, width = tokens.shape
    slots = picks.shape[2]
    hidden = w_in.shape[2]
    dec_rows, q_width = queries.shape
    lanes = 128 * pl.cdiv((dec_rows // 8) * 2 * HEADS, 128)
    anywhere = pl.BlockSpec(memory_space=pl.ANY)
    dma = pltpu.SemaphoreType.DMA
    vmem = pl.BlockSpec(memory_space=pltpu.VMEM)
    room = 2 * (rows * width + dec_rows * width)
    encoded, dec = pl.pallas_call(
        functools.partial(kernel, n_e, n_s),
        out_shape=(
            pltpu.VMEM((rows, width), BF16),
            pltpu.VMEM((dec_rows, width), BF16),
        ),
        in_specs=[anywhere] * 12,
        out_specs=(vmem, vmem),
        scratch_shapes=[
            pltpu.VMEM((rows, width), BF16),
            pltpu.VMEM(picks.shape, jnp.int32),
            pltpu.VMEM(gates.shape, F32),
            pltpu.VMEM(counts.shape, jnp.int32),
            pltpu.VMEM((2, 1, width), F32),
            pltpu.VMEM((width, hidden), BF16),
            pltpu.VMEM((hidden, width), BF16),
            pltpu.VMEM((2, width, q_width), BF16),
            pltpu.VMEM((q_width, width), BF16),
            pltpu.VMEM((n_s, dec_rows, q_width), BF16),
            pltpu.VMEM((n_e, slots, width), BF16),
            pltpu.VMEM((n_e + 1, slots, width), BF16),
            pltpu.VMEM((n_e + 1, slots, width), BF16),
            pltpu.VMEM((n_e, slots, width), BF16),
            pltpu.VMEM((n_s, dec_rows, q_width), BF16),
            pltpu.VMEM((n_s, dec_rows, q_width), BF16),
            pltpu.VMEM((n_s, 8, lanes), F32),
            pltpu.VMEM((n_s, 8, lanes), F32),
            pltpu.VMEM((n_s, dec_rows, q_width), F32),
            dma((10,)),
            dma((1,)),
            dma((n_e + 1,)),
            dma((2,)),
            dma((1,)),
            dma((1,)),
            dma((1,)),
            dma((1,)),
            dma((1,)),
            dma((1,)),
            dma((1,)),
        ],
        compiler_params=pltpu.CompilerParams(
            collective_id=0, has_side_effects=True, vmem_limit_bytes=VMEM_BYTES - room
        ),
    )(
        tokens,
        picks,
        gates,
        counts,
        norm_in.reshape(1, -1),
        norm_out.reshape(1, -1),
        w_in,
        w_out,
        w_key,
        w_value,
        queries,
        w_proj,
    )
    return pl.pallas_call(
        finish,
        out_shape=(
            jax.ShapeDtypeStruct((rows, width), BF16),
            jax.ShapeDtypeStruct((dec_rows, width), BF16),
        ),
        in_specs=[vmem] * 2,
        out_specs=(anywhere, anywhere),
        scratch_shapes=[dma((2,))],
        compiler_params=pltpu.CompilerParams(vmem_limit_bytes=8 * 2**20),
    )(encoded, dec)


def solution(mesh):
    in_specs = (
        P(("dp", "expert", "seq"), None),
        P(("dp", "expert", "seq"), None, None),
        P(("dp", "expert", "seq"), None, None),
        P(("dp", "expert", "seq"), None),
        P(),
        P(),
        P("expert", None, None),
        P("expert", None, None),
        P(),
        P(),
        P(("dp", "expert", "seq"), None),
        P(),
    )
    out_specs = (P(("dp", "expert", "seq"), None), P(("dp", "expert", "seq"), None))
    body = functools.partial(local, mesh.shape["expert"], mesh.shape["seq"])
    return jax.shard_map(body, mesh=mesh, in_specs=in_specs, out_specs=out_specs, check_vma=False)
```

```python
import functools

import jax
import jax.numpy as jnp
from jax import lax
from jax.experimental import pallas as pl
from jax.experimental.pallas import tpu as pltpu
from jax.sharding import PartitionSpec as P

HEADS = 8
EPSILON = 1e-06
VMEM_BYTES = 67043328
MESH = pl.DeviceIdType.MESH
F32 = jnp.float32
BF16 = jnp.bfloat16


def rms_norm(values, gain):
    mean_square = jnp.mean(values * values, axis=-1, keepdims=True)
    return values * lax.rsqrt(mean_square + EPSILON) * gain


def gelu(v):
    return 0.5 * v * (1.0 + jnp.tanh(0.7978845608028654 * (v + 0.044715 * v * v * v)))


def peer(n, at, r):
    upper = lax.div(2 * at, n)
    down = n - 1 - r
    return upper * (r + lax.div(r + n - at, n)) + (1 - upper) * (down - lax.div(at + n - down, n))


def rank(n, at, other):
    upper = lax.div(2 * at, n)
    above = lax.div(other + n - 1 - at, n)
    below = lax.div(at + n - 1 - other, n)
    return upper * (other - above) + (1 - upper) * (n - 1 - other - below)


def kernel(
    n_e,
    n_s,
    tokens_h,
    picks_h,
    gates_h,
    counts_h,
    norm_in_h,
    norm_out_h,
    w_in_h,
    w_out_h,
    w_key_h,
    w_value_h,
    queries_h,
    w_proj_h,
    enc_v,
    dec_v,
    tokens_v,
    picks_v,
    gates_v,
    counts_v,
    norms_v,
    w_in_v,
    w_out_v,
    w_kv_v,
    w_proj_v,
    q_v,
    send_a,
    recv_a,
    send_b,
    recv_b,
    part_v,
    part_r,
    stat_v,
    stat_r,
    spread_v,
    load_sem,
    a_send,
    a_recv,
    b_send,
    b_recv,
    q_send,
    q_recv,
    p_send,
    p_recv,
    t_send,
    t_recv,
):
    me_e = lax.axis_index("expert")
    me_s = lax.axis_index("seq")
    helper = lax.rem(me_s, 2)
    rows, width = tokens_v.shape
    slots = send_a.shape[1]
    dec_rows = q_v.shape[1]
    q_width = q_v.shape[2]
    head = q_width // HEADS
    own, far, extra = n_e - 2, n_e - 1, n_e

    loads = {}
    for i, (name, src, dst) in enumerate(
        (
            ("tokens", tokens_h, tokens_v),
            ("picks", picks_h, picks_v),
            ("queries", queries_h, q_v.at[me_s]),
            ("w_in", w_in_h.at[0], w_in_v),
            ("w_out", w_out_h.at[0], w_out_v),
            ("gates", gates_h, gates_v),
            ("counts", counts_h, counts_v),
            ("w_proj", w_proj_h, w_proj_v),
        )
    ):
        loads[name] = pltpu.make_async_copy(src, dst, load_sem.at[i])
    pairs = {}
    for i, (name, parts, dst) in enumerate(
        (("norms", (norm_in_h, norm_out_h), norms_v), ("w_kv", (w_key_h, w_value_h), w_kv_v))
    ):
        sem = load_sem.at[len(loads) + i]
        pairs[name] = [
            pltpu.make_async_copy(part, dst.at[k], sem) for k, part in enumerate(parts)
        ]
    both = {
        name: pltpu.make_async_copy(dst, dst, load_sem.at[len(loads) + i])
        for i, (name, dst) in enumerate((("norms", norms_v), ("w_kv", w_kv_v)))
    }
    loads["tokens"].start()
    loads["picks"].start()
    for copy in pairs["norms"]:
        copy.start()

    barrier = pltpu.get_barrier_semaphore()

    def greet(e, s):
        pl.semaphore_signal(
            barrier, inc=1, device_id={"expert": e, "seq": s}, device_id_type=MESH
        )

    @pl.when(helper == 1)
    def _():
        greet(peer(n_e, me_e, 0), me_s - 1)
        greet(peer(n_e, me_e, 0), me_s)

    for r in range(1, n_e - 1):
        greet(peer(n_e, me_e, r), me_s)
    for d in range(1, n_s):
        greet(me_e, lax.rem(me_s + d, n_s))
    for name in ("queries", "w_in", "w_out", "gates", "counts"):
        loads[name].start()
    for copy in pairs["w_kv"]:
        copy.start()
    loads["w_proj"].start()

    def remote(src, dst, send, recv, e, s):
        return pltpu.make_async_remote_copy(
            src_ref=src,
            dst_ref=dst,
            send_sem=send,
            recv_sem=recv,
            device_id={"expert": e, "seq": s},
            device_id_type=MESH,
        )

    def copy_a(r):
        to = peer(n_e, me_e, r)
        place = rank(n_e, to, me_e)
        first = lax.div(n_e - place, n_e)
        aside = first * (1 - helper)
        slot = (1 - first) * (place - 1) + first * far + aside
        return remote(
            send_a.at[to], recv_a.at[slot], a_send.at[0], a_recv.at[slot], to, me_s + aside
        )

    def copy_b(slot):
        aside = 1 if slot == extra else 0
        return remote(
            send_b.at[slot],
            recv_b.at[me_e],
            b_send.at[1 if slot >= far else 0],
            b_recv.at[0],
            peer(n_e, me_e, 0 if slot >= far else slot + 1),
            me_s - aside,
        )

    def whole(ref, first, many, sem):
        piece = ref.at[pl.ds(first, many)]
        return pltpu.make_async_copy(piece, piece, sem)

    def copy_q(d):
        to = lax.rem(me_s + d, n_s)
        return remote(q_v.at[me_s], q_v.at[me_s], q_send.at[0], q_recv.at[0], me_e, to)

    def copy_p(d):
        to = lax.rem(me_s + d, n_s)
        return remote(part_v.at[to], part_r.at[d], p_send.at[0], p_recv.at[0], me_e, to)

    def copy_t(d):
        to = lax.rem(me_s + d, n_s)
        return remote(stat_v.at[to], stat_r.at[d], t_send.at[0], t_recv.at[0], me_e, to)

    a_copies = [copy_a(r) for r in range(n_e - 1)]
    loads["tokens"].wait()
    both["norms"].wait()
    loads["picks"].wait()
    normed = rms_norm(tokens_v[...].astype(F32), norms_v[0]).astype(BF16)
    pick_row = jnp.concatenate([picks_v[0, j : j + 1, :] for j in range(n_e)], axis=1)
    position = lax.broadcasted_iota(jnp.int32, (rows, n_e * slots), 0)
    chosen = jnp.where(position == pick_row, 1.0, 0.0).astype(BF16)
    send_a[...] = (
        lax.dot_general(chosen, normed, (((0,), (0,)), ((), ())), preferred_element_type=F32)
        .astype(BF16)
        .reshape(n_e, slots, width)
    )
    pl.semaphore_wait(barrier, n_e - 1 + n_s - 1)
    for copy in a_copies:
        copy.start()
    loads["queries"].wait()
    for d in range(1, n_s):
        copy_q(d).start()
    recv_a[own] = send_a[me_e]

    loads["gates"].wait()
    loads["counts"].wait()
    slot_lane = lax.broadcasted_iota(jnp.int32, (1, slots), 1)
    gate_row = jnp.concatenate(
        [
            jnp.where(slot_lane < counts_v[0:1, j : j + 1], gates_v[0, j : j + 1, :], 0.0)
            for j in range(n_e)
        ],
        axis=1,
    )
    high = gate_row.astype(BF16).astype(F32)
    middle = (gate_row - high).astype(BF16).astype(F32)
    low = gate_row - high - middle
    gate_three = jnp.concatenate([high, middle, low], axis=1)
    pick_three = jnp.concatenate([pick_row] * 3, axis=1)
    position_three = lax.broadcasted_iota(jnp.int32, (rows, 3 * n_e * slots), 0)
    combine = jnp.where(position_three == pick_three, gate_three, 0.0).astype(BF16)

    def feed(first, many):
        flat = recv_a[first : first + many].reshape(many * slots, width)
        hidden = gelu(jnp.dot(flat, w_in_v[...], preferred_element_type=F32)).astype(BF16)
        result = jnp.dot(hidden, w_out_v[...], preferred_element_type=F32).astype(BF16)
        send_b[first : first + many] = result.reshape(many, slots, width)

    loads["w_in"].wait()
    loads["w_out"].wait()
    feed(own, 1)
    recv_b[me_e] = send_b[own]
    near = [whole(recv_a, slot, 1, a_recv.at[slot]) for slot in range(own)]
    far_own = whole(recv_a, far, 1, a_recv.at[far])
    far_aside = whole(recv_a, extra, 1, a_recv.at[extra])
    upper = lax.div(2 * me_e, n_e)

    def feed_far():
        for slot, copy in ((far, far_own), (extra, far_aside)):
            copy.wait()
            feed(slot, 1)
            copy_b(slot).start()

    @pl.when(helper == 0)
    def _():
        for slot in reversed(range(own)):
            near[slot].wait()
            feed(slot, 1)
            copy_b(slot).start()

    @pl.when(helper * upper == 1)
    def _():
        feed_far()

    @pl.when(helper == 1)
    def _():
        for copy in near:
            copy.wait()
        feed(0, own)
        for slot in range(own):
            copy_b(slot).start()

    @pl.when(helper * (1 - upper) == 1)
    def _():
        feed_far()

    both["w_kv"].wait()
    whole(q_v, 0, n_s - 1, q_recv.at[0]).wait()
    all_rows = n_s * dec_rows
    queries = q_v[...].reshape(all_rows, q_width)
    whole(recv_b, 0, n_e - 1, b_recv.at[0]).wait()
    returned = recv_b[...].reshape(n_e * slots, width)
    expert_sum = jnp.dot(
        combine, jnp.concatenate([returned] * 3, axis=0), preferred_element_type=F32
    )
    mixed = tokens_v[...].astype(F32) + expert_sum
    encoded = rms_norm(mixed, norms_v[1]).astype(BF16)
    enc_v[...] = encoded
    slab = min(256, q_width)
    groups = q_width // slab
    group = slab // head
    lanes = stat_v.shape[2]
    lane_head = lax.broadcasted_iota(jnp.int32, (1, slab), 1) // head
    stat_lane = lax.broadcasted_iota(jnp.int32, (1, lanes), 1)
    bands = dec_rows // 8
    only = [jnp.where(lane_head == h, 1.0, 0.0).astype(BF16) for h in range(group)]
    slabs = [slice(g * slab, (g + 1) * slab) for g in range(groups)]
    keys = jnp.dot(encoded, w_kv_v[0], preferred_element_type=F32).astype(BF16)
    scores = []
    for cols in slabs:
        key_heads = jnp.concatenate([keys[:, cols] * m for m in only], axis=0)
        scores.append(
            lax.dot_general(
                queries[:, cols], key_heads, (((1,), (1,)), ((), ())), preferred_element_type=F32
            )
            * (head**-0.5)
        )
    values = jnp.dot(encoded, w_kv_v[1], preferred_element_type=F32).astype(BF16)
    tops, totals = [], []
    for cols, score in zip(slabs, scores):
        weights = []
        for h in range(group):
            span = score[:, h * rows : (h + 1) * rows]
            row_max = jnp.max(span, axis=1, keepdims=True)
            weight = jnp.exp(span - row_max)
            tops.append(row_max)
            totals.append(jnp.sum(weight, axis=1, keepdims=True))
            weights.append(weight.astype(BF16))
        value_heads = jnp.concatenate([values[:, cols] * m for m in only], axis=0)
        product = jnp.dot(
            jnp.concatenate(weights, axis=1), value_heads, preferred_element_type=F32
        )
        part_v[:, :, cols] = product.astype(BF16).reshape(n_s, dec_rows, slab)
    for s in range(n_s):
        packed = jnp.zeros((8, lanes), F32)
        for band in range(bands):
            at = s * dec_rows + band * 8
            piece = jnp.zeros((8, lanes), F32)
            for h in range(HEADS):
                lane = band * 2 * HEADS + h
                piece = jnp.where(stat_lane == lane, tops[h][at : at + 8], piece)
                piece = jnp.where(stat_lane == lane + HEADS, totals[h][at : at + 8], piece)
            packed = packed + piece
        stat_v[s] = packed
    for d in range(1, n_s):
        copy_t(d).start()
        copy_p(d).start()
    part_r[0] = part_v[me_s]
    stat_r[0] = stat_v[me_s]

    whole(send_a, 0, n_e - 1, a_send.at[0]).wait()
    whole(send_b, 0, own, b_send.at[0]).wait()

    @pl.when(helper == 1)
    def _():
        whole(send_b, far, 2, b_send.at[1]).wait()

    whole(q_v, 0, n_s - 1, q_send.at[0]).wait()
    loads["w_proj"].wait()
    whole(stat_r, 1, n_s - 1, t_recv.at[0]).wait()
    stat = []
    for d in range(n_s):
        packed = stat_r[d]
        stat.append(
            jnp.concatenate(
                [
                    pltpu.roll(packed, lanes - band * 2 * HEADS, 1) if band else packed
                    for band in range(bands)
                ],
                axis=0,
            )
        )
    top = functools.reduce(jnp.maximum, stat)
    factor = [jnp.exp(s - top)[:, :HEADS] for s in stat]
    total = sum(f * s[:, HEADS : 2 * HEADS] for f, s in zip(factor, stat))
    for d in range(n_s):
        scale = factor[d] / total
        for g, cols in enumerate(slabs):
            at = g * group
            spread = jnp.broadcast_to(scale[:, at : at + 1], (dec_rows, slab))
            for h in range(1, group):
                spread = jnp.where(lane_head == h, scale[:, at + h : at + h + 1], spread)
            spread_v[d, :, cols] = spread
    whole(stat_v, 0, n_s - 1, t_send.at[0]).wait()
    whole(part_v, 0, n_s - 1, p_send.at[0]).wait()
    whole(part_r, 1, n_s - 1, p_recv.at[0]).wait()
    summed = sum(spread_v[d] * part_r[d].astype(F32) for d in range(n_s))
    dec_v[...] = jnp.dot(
        summed.astype(BF16), w_proj_v[...], preferred_element_type=F32
    ).astype(BF16)


def finish(enc_v, dec_v, encoded_h, dec_h, store_sem):
    enc_store = pltpu.make_async_copy(enc_v, encoded_h, store_sem.at[0])
    dec_store = pltpu.make_async_copy(dec_v, dec_h, store_sem.at[1])
    enc_store.start()
    dec_store.start()
    enc_store.wait()
    dec_store.wait()


def local(
    n_e,
    n_s,
    tokens,
    picks,
    gates,
    counts,
    norm_in,
    norm_out,
    w_in,
    w_out,
    w_key,
    w_value,
    queries,
    w_proj,
):
    rows, width = tokens.shape
    slots = picks.shape[2]
    hidden = w_in.shape[2]
    dec_rows, q_width = queries.shape
    lanes = 128 * pl.cdiv((dec_rows // 8) * 2 * HEADS, 128)
    anywhere = pl.BlockSpec(memory_space=pl.ANY)
    dma = pltpu.SemaphoreType.DMA
    vmem = pl.BlockSpec(memory_space=pltpu.VMEM)
    room = 2 * (rows * width + dec_rows * width)
    encoded, dec = pl.pallas_call(
        functools.partial(kernel, n_e, n_s),
        out_shape=(
            pltpu.VMEM((rows, width), BF16),
            pltpu.VMEM((dec_rows, width), BF16),
        ),
        in_specs=[anywhere] * 12,
        out_specs=(vmem, vmem),
        scratch_shapes=[
            pltpu.VMEM((rows, width), BF16),
            pltpu.VMEM(picks.shape, jnp.int32),
            pltpu.VMEM(gates.shape, F32),
            pltpu.VMEM(counts.shape, jnp.int32),
            pltpu.VMEM((2, 1, width), F32),
            pltpu.VMEM((width, hidden), BF16),
            pltpu.VMEM((hidden, width), BF16),
            pltpu.VMEM((2, width, q_width), BF16),
            pltpu.VMEM((q_width, width), BF16),
            pltpu.VMEM((n_s, dec_rows, q_width), BF16),
            pltpu.VMEM((n_e, slots, width), BF16),
            pltpu.VMEM((n_e + 1, slots, width), BF16),
            pltpu.VMEM((n_e + 1, slots, width), BF16),
            pltpu.VMEM((n_e, slots, width), BF16),
            pltpu.VMEM((n_s, dec_rows, q_width), BF16),
            pltpu.VMEM((n_s, dec_rows, q_width), BF16),
            pltpu.VMEM((n_s, 8, lanes), F32),
            pltpu.VMEM((n_s, 8, lanes), F32),
            pltpu.VMEM((n_s, dec_rows, q_width), F32),
            dma((10,)),
            dma((1,)),
            dma((n_e + 1,)),
            dma((2,)),
            dma((1,)),
            dma((1,)),
            dma((1,)),
            dma((1,)),
            dma((1,)),
            dma((1,)),
            dma((1,)),
        ],
        compiler_params=pltpu.CompilerParams(
            collective_id=0, has_side_effects=True, vmem_limit_bytes=VMEM_BYTES - room
        ),
    )(
        tokens,
        picks,
        gates,
        counts,
        norm_in.reshape(1, -1),
        norm_out.reshape(1, -1),
        w_in,
        w_out,
        w_key,
        w_value,
        queries,
        w_proj,
    )
    return pl.pallas_call(
        finish,
        out_shape=(
            jax.ShapeDtypeStruct((rows, width), BF16),
            jax.ShapeDtypeStruct((dec_rows, width), BF16),
        ),
        in_specs=[vmem] * 2,
        out_specs=(anywhere, anywhere),
        scratch_shapes=[dma((2,))],
        compiler_params=pltpu.CompilerParams(vmem_limit_bytes=8 * 2**20),
    )(encoded, dec)


def solution(mesh):
    in_specs = (
        P(("dp", "expert", "seq"), None),
        P(("dp", "expert", "seq"), None, None),
        P(("dp", "expert", "seq"), None, None),
        P(("dp", "expert", "seq"), None),
        P(),
        P(),
        P("expert", None, None),
        P("expert", None, None),
        P(),
        P(),
        P(("dp", "expert", "seq"), None),
        P(),
    )
    out_specs = (P(("dp", "expert", "seq"), None), P(("dp", "expert", "seq"), None))
    body = functools.partial(local, mesh.shape["expert"], mesh.shape["seq"])
    return jax.shard_map(body, mesh=mesh, in_specs=in_specs, out_specs=out_specs, check_vma=False)
```

```python
import functools
import math

import jax
import jax.numpy as jnp
from jax import lax
from jax.experimental import pallas as pl
from jax.experimental.pallas import tpu as pltpu
from jax.sharding import PartitionSpec as P

HEADS = 8
EPSILON = 1e-06
VMEM_BYTES = 67043328
MESH = pl.DeviceIdType.MESH
F32 = jnp.float32
BF16 = jnp.bfloat16


def rms_norm(values, gain):
    mean_square = jnp.mean(values * values, axis=-1, keepdims=True)
    return values * lax.rsqrt(mean_square + EPSILON) * gain


def gelu(v):
    return 0.5 * v * (1.0 + jnp.tanh(0.7978845608028654 * (v + 0.044715 * v * v * v)))


def peer(n, at, r):
    upper = lax.div(2 * at, n)
    down = n - 1 - r
    return upper * (r + lax.div(r + n - at, n)) + (1 - upper) * (down - lax.div(at + n - down, n))


def rank(n, at, other):
    upper = lax.div(2 * at, n)
    above = lax.div(other + n - 1 - at, n)
    below = lax.div(at + n - 1 - other, n)
    return upper * (other - above) + (1 - upper) * (n - 1 - other - below)


def kernel(
    n_e,
    n_s,
    tokens_h,
    picks_h,
    gates_h,
    counts_h,
    norm_in_h,
    norm_out_h,
    w_in_h,
    w_out_h,
    w_key_h,
    w_value_h,
    queries_h,
    w_proj_h,
    enc_v,
    dec_v,
    tokens_v,
    picks_v,
    gates_v,
    counts_v,
    norms_v,
    w_in_v,
    w_out_v,
    w_kv_v,
    w_proj_v,
    q_v,
    send_a,
    recv_a,
    send_b,
    recv_b,
    part_v,
    part_r,
    stat_v,
    stat_r,
    spread_v,
    load_sem,
    a_send,
    a_recv,
    b_recv,
    q_recv,
    p_send,
    p_recv,
    t_send,
    t_recv,
):
    me_e = lax.axis_index("expert")
    me_s = lax.axis_index("seq")
    helper = lax.rem(me_s, 2)
    rows, width = tokens_v.shape
    slots = send_a.shape[1]
    dec_rows = q_v.shape[1]
    q_width = q_v.shape[2]
    head = q_width // HEADS
    own, far, extra = n_e - 2, n_e - 1, n_e

    loads = {}
    for i, (name, src, dst) in enumerate(
        (
            ("tokens", tokens_h, tokens_v),
            ("picks", picks_h, picks_v),
            ("queries", queries_h, q_v.at[me_s]),
            ("w_in", w_in_h.at[0], w_in_v),
            ("w_out", w_out_h.at[0], w_out_v),
            ("gates", gates_h, gates_v),
            ("counts", counts_h, counts_v),
            ("w_proj", w_proj_h, w_proj_v),
        )
    ):
        loads[name] = pltpu.make_async_copy(src, dst, load_sem.at[i])
    pairs = {}
    for i, (name, parts, dst) in enumerate(
        (("norms", (norm_in_h, norm_out_h), norms_v), ("w_kv", (w_key_h, w_value_h), w_kv_v))
    ):
        sem = load_sem.at[len(loads) + i]
        pairs[name] = [
            pltpu.make_async_copy(part, dst.at[k], sem) for k, part in enumerate(parts)
        ]
    both = {
        name: pltpu.make_async_copy(dst, dst, load_sem.at[len(loads) + i])
        for i, (name, dst) in enumerate((("norms", norms_v), ("w_kv", w_kv_v)))
    }
    loads["tokens"].start()
    loads["picks"].start()
    for copy in pairs["norms"]:
        copy.start()

    barrier = pltpu.get_barrier_semaphore()

    def greet(e, s):
        pl.semaphore_signal(
            barrier, inc=1, device_id={"expert": e, "seq": s}, device_id_type=MESH
        )

    @pl.when(helper == 1)
    def _():
        greet(peer(n_e, me_e, 0), me_s - 1)
        greet(peer(n_e, me_e, 0), me_s)

    for r in range(1, n_e - 1):
        greet(peer(n_e, me_e, r), me_s)
    for d in range(1, n_s):
        greet(me_e, lax.rem(me_s + d, n_s))
    for name in ("queries", "w_in", "w_out", "gates", "counts"):
        loads[name].start()
    for copy in pairs["w_kv"]:
        copy.start()
    loads["w_proj"].start()

    def remote(src, dst, send, recv, e, s):
        return pltpu.make_async_remote_copy(
            src_ref=src,
            dst_ref=dst,
            send_sem=send,
            recv_sem=recv,
            device_id={"expert": e, "seq": s},
            device_id_type=MESH,
        )

    def copy_a(r):
        to = peer(n_e, me_e, r)
        place = rank(n_e, to, me_e)
        first = lax.div(n_e - place, n_e)
        aside = first * (1 - helper)
        slot = (1 - first) * (place - 1) + first * far + aside
        return remote(
            send_a.at[to], recv_a.at[slot], a_send.at[0], a_recv.at[slot], to, me_s + aside
        )

    def copy_b(slot):
        aside = 1 if slot == extra else 0
        return remote(
            send_b.at[slot],
            recv_b.at[me_e],
            a_send.at[0],
            b_recv.at[0],
            peer(n_e, me_e, 0 if slot >= far else slot + 1),
            me_s - aside,
        )

    def whole(ref, first, many, sem):
        piece = ref.at[pl.ds(first, many)]
        return pltpu.make_async_copy(piece, piece, sem)

    def copy_q(d):
        to = lax.rem(me_s + d, n_s)
        return remote(q_v.at[me_s], q_v.at[me_s], a_send.at[0], q_recv.at[0], me_e, to)

    def copy_p(d):
        to = lax.rem(me_s + d, n_s)
        return remote(part_v.at[to], part_r.at[d], p_send.at[0], p_recv.at[0], me_e, to)

    def copy_t(d):
        to = lax.rem(me_s + d, n_s)
        return remote(stat_v.at[to], stat_r.at[d], t_send.at[0], t_recv.at[0], me_e, to)

    a_copies = [copy_a(r) for r in range(n_e - 1)]
    loads["tokens"].wait()
    both["norms"].wait()
    loads["picks"].wait()
    normed = rms_norm(tokens_v[...].astype(F32), norms_v[0]).astype(BF16)
    pick_row = jnp.concatenate([picks_v[0, j : j + 1, :] for j in range(n_e)], axis=1)
    position = lax.broadcasted_iota(jnp.int32, (rows, n_e * slots), 0)
    chosen = jnp.where(position == pick_row, 1.0, 0.0).astype(BF16)
    send_a[...] = (
        lax.dot_general(chosen, normed, (((0,), (0,)), ((), ())), preferred_element_type=F32)
        .astype(BF16)
        .reshape(n_e, slots, width)
    )
    pl.semaphore_wait(barrier, n_e - 1 + n_s - 1)
    for copy in a_copies:
        copy.start()
    loads["queries"].wait()
    for d in range(1, n_s):
        copy_q(d).start()
    recv_a[own] = send_a[me_e]

    loads["gates"].wait()
    loads["counts"].wait()
    slot_lane = lax.broadcasted_iota(jnp.int32, (1, slots), 1)
    gate_row = jnp.concatenate(
        [
            jnp.where(slot_lane < counts_v[0:1, j : j + 1], gates_v[0, j : j + 1, :], 0.0)
            for j in range(n_e)
        ],
        axis=1,
    )
    high = gate_row.astype(BF16).astype(F32)
    middle = (gate_row - high).astype(BF16).astype(F32)
    low = gate_row - high - middle
    gate_three = jnp.concatenate([high, middle, low], axis=1)
    pick_three = jnp.concatenate([pick_row] * 3, axis=1)
    position_three = lax.broadcasted_iota(jnp.int32, (rows, 3 * n_e * slots), 0)
    combine = jnp.where(position_three == pick_three, gate_three, 0.0).astype(BF16)

    def feed(first, many):
        flat = recv_a[first : first + many].reshape(many * slots, width)
        hidden = gelu(jnp.dot(flat, w_in_v[...], preferred_element_type=F32)).astype(BF16)
        result = jnp.dot(hidden, w_out_v[...], preferred_element_type=F32).astype(BF16)
        send_b[first : first + many] = result.reshape(many, slots, width)

    loads["w_in"].wait()
    loads["w_out"].wait()
    feed(own, 1)
    recv_b[me_e] = send_b[own]
    near = [whole(recv_a, slot, 1, a_recv.at[slot]) for slot in range(own)]
    far_own = whole(recv_a, far, 1, a_recv.at[far])
    far_aside = whole(recv_a, extra, 1, a_recv.at[extra])
    upper = lax.div(2 * me_e, n_e)

    def feed_far():
        for slot, copy in ((far, far_own), (extra, far_aside)):
            copy.wait()
            feed(slot, 1)
            copy_b(slot).start()

    @pl.when(helper == 0)
    def _():
        for slot in reversed(range(own)):
            near[slot].wait()
            feed(slot, 1)
            copy_b(slot).start()

    @pl.when(helper * upper == 1)
    def _():
        feed_far()

    @pl.when(helper == 1)
    def _():
        for slot in reversed(range(own)):
            near[slot].wait()
            feed(slot, 1)
            copy_b(slot).start()

    @pl.when(helper * (1 - upper) == 1)
    def _():
        feed_far()

    both["w_kv"].wait()
    whole(q_v, 0, n_s - 1, q_recv.at[0]).wait()
    all_rows = n_s * dec_rows
    queries = q_v[...].reshape(all_rows, q_width)
    whole(recv_b, 0, n_e - 1, b_recv.at[0]).wait()
    returned = recv_b[...].reshape(n_e * slots, width)
    expert_sum = jnp.dot(
        combine, jnp.concatenate([returned] * 3, axis=0), preferred_element_type=F32
    )
    mixed = tokens_v[...].astype(F32) + expert_sum
    encoded = rms_norm(mixed, norms_v[1]).astype(BF16)
    enc_v[...] = encoded
    slab = min(256, q_width)
    groups = q_width // slab
    group = slab // head
    lanes = stat_v.shape[2]
    lane_head = lax.broadcasted_iota(jnp.int32, (1, slab), 1) // head
    stat_lane = lax.broadcasted_iota(jnp.int32, (1, lanes), 1)
    bands = dec_rows // 8
    only = [jnp.where(lane_head == h, 1.0, 0.0).astype(BF16) for h in range(group)]
    slabs = [slice(g * slab, (g + 1) * slab) for g in range(groups)]
    keys = jnp.dot(encoded, w_kv_v[0], preferred_element_type=F32).astype(BF16)
    values = jnp.dot(encoded, w_kv_v[1], preferred_element_type=F32).astype(BF16)
    scores = []
    for cols in slabs:
        key_heads = jnp.concatenate([keys[:, cols] * m for m in only], axis=0)
        scores.append(
            lax.dot_general(
                queries[:, cols], key_heads, (((1,), (1,)), ((), ())), preferred_element_type=F32
            )
        )
    sharpness = head**-0.5 * math.log2(math.e)
    tops, totals = [], []
    for cols, score in zip(slabs, scores):
        weights = []
        for h in range(group):
            span = score[:, h * rows : (h + 1) * rows]
            row_max = jnp.max(span, axis=1, keepdims=True)
            weight = jnp.exp2((span - row_max) * sharpness)
            tops.append(row_max)
            totals.append(jnp.sum(weight, axis=1, keepdims=True))
            weights.append(weight.astype(BF16))
        value_heads = jnp.concatenate([values[:, cols] * m for m in only], axis=0)
        product = jnp.dot(
            jnp.concatenate(weights, axis=1), value_heads, preferred_element_type=F32
        )
        part_v[:, :, cols] = product.astype(BF16).reshape(n_s, dec_rows, slab)
    for s in range(n_s):
        packed = jnp.zeros((8, lanes), F32)
        for band in range(bands):
            at = s * dec_rows + band * 8
            piece = jnp.zeros((8, lanes), F32)
            for h in range(HEADS):
                lane = band * 2 * HEADS + h
                piece = jnp.where(stat_lane == lane, tops[h][at : at + 8], piece)
                piece = jnp.where(stat_lane == lane + HEADS, totals[h][at : at + 8], piece)
            packed = packed + piece
        stat_v[s] = packed
    for k in range(1, n_s // 2):
        for core in range(2):
            to = 2 * lax.rem(lax.div(me_s, 2) + k, n_s // 2) + core
            d = lax.rem(to - me_s + n_s, n_s)
            copy_t(d).start()
            copy_p(d).start()
    d = lax.rem(n_s + 1 - 2 * helper, n_s)
    copy_t(d).start()
    copy_p(d).start()
    part_r[0] = part_v[me_s]
    stat_r[0] = stat_v[me_s]

    sent = ((n_e - 1 + own) * slots * width + (n_s - 1) * dec_rows * q_width) // width

    @pl.when(helper == 0)
    def _():
        whole(w_out_v, 0, sent, a_send.at[0]).wait()

    @pl.when(helper == 1)
    def _():
        whole(w_out_v, 0, sent + 2 * slots, a_send.at[0]).wait()

    loads["w_proj"].wait()
    whole(stat_r, 1, n_s - 1, t_recv.at[0]).wait()
    stat = []
    for d in range(n_s):
        packed = stat_r[d]
        stat.append(
            jnp.concatenate(
                [
                    pltpu.roll(packed, lanes - band * 2 * HEADS, 1) if band else packed
                    for band in range(bands)
                ],
                axis=0,
            )
        )
    top = functools.reduce(jnp.maximum, stat)
    factor = [jnp.exp2((s - top) * sharpness)[:, :HEADS] for s in stat]
    total = sum(f * s[:, HEADS : 2 * HEADS] for f, s in zip(factor, stat))
    for d in range(n_s):
        scale = factor[d] / total
        for g, cols in enumerate(slabs):
            at = g * group
            spread = jnp.broadcast_to(scale[:, at : at + 1], (dec_rows, slab))
            for h in range(1, group):
                spread = jnp.where(lane_head == h, scale[:, at + h : at + h + 1], spread)
            spread_v[d, :, cols] = spread
    whole(stat_v, 0, n_s - 1, t_send.at[0]).wait()
    whole(part_v, 0, n_s - 1, p_send.at[0]).wait()
    whole(part_r, 1, n_s - 1, p_recv.at[0]).wait()
    summed = sum(spread_v[d] * part_r[d].astype(F32) for d in range(n_s))
    dec_v[...] = jnp.dot(
        summed.astype(BF16), w_proj_v[...], preferred_element_type=F32
    ).astype(BF16)


def finish(enc_v, dec_v, encoded_h, dec_h, store_sem):
    enc_store = pltpu.make_async_copy(enc_v, encoded_h, store_sem.at[0])
    dec_store = pltpu.make_async_copy(dec_v, dec_h, store_sem.at[1])
    enc_store.start()
    dec_store.start()
    enc_store.wait()
    dec_store.wait()


def local(
    n_e,
    n_s,
    tokens,
    picks,
    gates,
    counts,
    norm_in,
    norm_out,
    w_in,
    w_out,
    w_key,
    w_value,
    queries,
    w_proj,
):
    rows, width = tokens.shape
    slots = picks.shape[2]
    hidden = w_in.shape[2]
    dec_rows, q_width = queries.shape
    lanes = 128 * pl.cdiv((dec_rows // 8) * 2 * HEADS, 128)
    anywhere = pl.BlockSpec(memory_space=pl.ANY)
    dma = pltpu.SemaphoreType.DMA
    vmem = pl.BlockSpec(memory_space=pltpu.VMEM)
    room = 2 * (rows * width + dec_rows * width)
    encoded, dec = pl.pallas_call(
        functools.partial(kernel, n_e, n_s),
        out_shape=(
            pltpu.VMEM((rows, width), BF16),
            pltpu.VMEM((dec_rows, width), BF16),
        ),
        in_specs=[anywhere] * 12,
        out_specs=(vmem, vmem),
        scratch_shapes=[
            pltpu.VMEM((rows, width), BF16),
            pltpu.VMEM(picks.shape, jnp.int32),
            pltpu.VMEM(gates.shape, F32),
            pltpu.VMEM(counts.shape, jnp.int32),
            pltpu.VMEM((2, 1, width), F32),
            pltpu.VMEM((width, hidden), BF16),
            pltpu.VMEM((hidden, width), BF16),
            pltpu.VMEM((2, width, q_width), BF16),
            pltpu.VMEM((q_width, width), BF16),
            pltpu.VMEM((n_s, dec_rows, q_width), BF16),
            pltpu.VMEM((n_e, slots, width), BF16),
            pltpu.VMEM((n_e + 1, slots, width), BF16),
            pltpu.VMEM((n_e + 1, slots, width), BF16),
            pltpu.VMEM((n_e, slots, width), BF16),
            pltpu.VMEM((n_s, dec_rows, q_width), BF16),
            pltpu.VMEM((n_s, dec_rows, q_width), BF16),
            pltpu.VMEM((n_s, 8, lanes), F32),
            pltpu.VMEM((n_s, 8, lanes), F32),
            pltpu.VMEM((n_s, dec_rows, q_width), F32),
            dma((10,)),
            dma((1,)),
            dma((n_e + 1,)),
            dma((1,)),
            dma((1,)),
            dma((1,)),
            dma((1,)),
            dma((1,)),
            dma((1,)),
        ],
        compiler_params=pltpu.CompilerParams(
            collective_id=0, has_side_effects=True, vmem_limit_bytes=VMEM_BYTES - room
        ),
    )(
        tokens,
        picks,
        gates,
        counts,
        norm_in.reshape(1, -1),
        norm_out.reshape(1, -1),
        w_in,
        w_out,
        w_key,
        w_value,
        queries,
        w_proj,
    )
    return pl.pallas_call(
        finish,
        out_shape=(
            jax.ShapeDtypeStruct((rows, width), BF16),
            jax.ShapeDtypeStruct((dec_rows, width), BF16),
        ),
        in_specs=[vmem] * 2,
        out_specs=(anywhere, anywhere),
        scratch_shapes=[dma((2,))],
        compiler_params=pltpu.CompilerParams(vmem_limit_bytes=8 * 2**20),
    )(encoded, dec)


def solution(mesh):
    in_specs = (
        P(("dp", "expert", "seq"), None),
        P(("dp", "expert", "seq"), None, None),
        P(("dp", "expert", "seq"), None, None),
        P(("dp", "expert", "seq"), None),
        P(),
        P(),
        P("expert", None, None),
        P("expert", None, None),
        P(),
        P(),
        P(("dp", "expert", "seq"), None),
        P(),
    )
    out_specs = (P(("dp", "expert", "seq"), None), P(("dp", "expert", "seq"), None))
    body = functools.partial(local, mesh.shape["expert"], mesh.shape["seq"])
    return jax.shard_map(body, mesh=mesh, in_specs=in_specs, out_specs=out_specs, check_vma=False)
```
